32 devices in a mesh: groups: 2 (over x), seq: 8 (over z, y), batch: 2 (over core).
Axes of the slice: x: 2, y: 2, z: 4, core: 2. Of those that a mesh axis runs over, the one named last changes fastest.
Arguments:
- prompt_cache: bfloat16 [16, 256, 8, 256], P(('groups', 'batch'), 'seq'), parts along dimension 0, may hold values from -6 to 6
- prompt_states: float32 [16, 8, 16, 16384], P(('groups', 'batch'), 'seq'), parts along dimension 0, may hold values from -6 to 6
- block_steps: float32 [16, 8, 16384], P(('groups', 'batch'), 'seq'), parts along dimension 0, may hold values from 0.005 to 0.1
- prompt_lengths: int32 [16], P('groups'), parts along dimension 0, may hold values from 42 to 255
- target_slots: int32 [16], P('groups'), parts along dimension 0, may hold values from 0 to 15, as said below
- cache_lengths: int32 [32], P(('groups', 'batch')), parts along dimension 0, may hold values from 42 to 255
- resident_cache: bfloat16 [32, 32, 8, 8, 256], P(('groups', 'batch'), None, 'seq'), parts along dimension 0, may hold values from -6 to 6
- token_cache: bfloat16 [32, 8, 256], P(('groups', 'batch')), parts along dimension 0, may hold values from -6 to 6
- queries: bfloat16 [32, 64, 128], P(('groups', 'batch')), parts along dimension 0, may hold values from -6 to 6
- resident_states: float32 [32, 16, 16384], P(('groups', 'batch'), None, 'seq'), parts along dimension 0, may hold values from -6 to 6
- decay_rates: float32 [16, 16384], replicated, may hold values from 0.05 to 10
- step_sizes: float32 [32, 16384], P(('groups', 'batch'), 'seq'), parts along dimension 0, may hold values from 0.01 to 1
- inner_input: bfloat16 [32, 16384], P(('groups', 'batch'), 'seq'), parts along dimension 0, may hold values from -6 to 6
- inner_gate: bfloat16 [32, 16384], P(('groups', 'batch'), 'seq'), parts along dimension 0, may hold values from -6 to 6
- state_input: float32 [32, 16], P(('groups', 'batch')), parts along dimension 0, may hold values from -6 to 6
- state_readout: float32 [32, 16], P(('groups', 'batch')), parts along dimension 0, may hold values from -6 to 6
- skip_gain: float32 [16384], P('seq'), may hold values from 0.5 to 1.5
Outputs:
- merged_cache: bfloat16 [32, 32, 8, 8, 256], P(('groups', 'batch'), None, 'seq'), parts along dimension 0
- attention: bfloat16 [32, 64, 128], P(('groups', 'batch'), 'seq'), parts along dimension 0
- next_states: float32 [32, 16, 16384], P(('groups', 'batch'), None, 'seq'), parts along dimension 0
- mamba_output: bfloat16 [32, 16384], P(('groups', 'batch'), 'seq'), parts along dimension 0
The draws below stay inside these ranges and needn't reach their ends.
There are 2 independent parts, one for each index of `groups`. The reference program is written for one: setup_inputs(seed, part) draws one part's arguments, and reference() takes and returns one part's arrays. A program takes and returns all parts, laid end to end along the dimension named above; an argument that names none is the same for every part. Nothing has to cross between parts.
Inputs may be any that keep to these rules, and one draw needn't show every extreme that they name: `target_slots`: 8 distinct slots.
All inputs are finite; a program needn't handle non-finite values.
Results may differ from the reference program's by a relative error of at most 0.0019.
Values may be sent and summed in bfloat16 or wider, within the bound.
A program may use at most 320 MiB of HBM per device.

```python
import math
import jax
import jax.numpy as jnp
from jax import lax

HEADS = 64
KV_HEADS = 8
HEAD_DIM = 128
INNER = 16384
STATE = 16
PROMPTS = 8
BLOCK_LEN = 32
SLOTS_DEV = 8
PROMPT_MAX = 256
SLOTS = 16
N_SEQ = 8
N_BATCH = 2


def draw_target_slots(key, part):
    shuffled = jax.random.permutation(key, SLOTS)
    return shuffled[:PROMPTS].astype(jnp.int32)


def sign_direction(key):
    return jax.random.rademacher(jax.random.fold_in(key, 7101), (KV_HEADS, HEAD_DIM), dtype=jnp.float32)


def key_amplitudes():
    return jnp.array([4.8, 4.76, 4.72], jnp.float32)


def keyed_cache(key, row_count, salt_value, level_set):
    kv_width = 2 * HEAD_DIM
    noise_key, spot_key, fine_key = jax.random.split(jax.random.fold_in(key, salt_value), 3)
    base_draw = jnp.clip(jax.random.normal(noise_key, (row_count, PROMPT_MAX, KV_HEADS, kv_width), jnp.float32), -6.0, 6.0)
    reach_len = max(PROMPT_MAX // 6, 3)

    def pick_spots(row_index):
        return jax.random.permutation(jax.random.fold_in(spot_key, row_index), reach_len)[:3].astype(jnp.int32)
    spot_rows = jax.vmap(pick_spots)(jnp.arange(row_count, dtype=jnp.int32))
    position = jnp.arange(PROMPT_MAX, dtype=jnp.int32)
    hit_table = (position[None, None, :] == spot_rows[:, :, None]).astype(jnp.float32)
    amplitude = jnp.einsum('rkt,k->rt', hit_table, level_set)
    chosen = jnp.sum(hit_table, axis=1)
    direction = sign_direction(key)
    fine_noise = 0.02 * jnp.clip(jax.random.normal(fine_key, (row_count, PROMPT_MAX, KV_HEADS, HEAD_DIM), jnp.float32), -3.0, 3.0)
    aligned = amplitude[:, :, None, None] * direction[None, None] + fine_noise
    new_keys = jnp.where(chosen[:, :, None, None] > 0.5, aligned, base_draw[..., :HEAD_DIM])
    return jnp.concatenate([new_keys, base_draw[..., HEAD_DIM:]], axis=3)


def draw_prompt_cache(key, part):
    level_set = key_amplitudes()
    return keyed_cache(key, PROMPTS, 11, level_set).astype(jnp.bfloat16)


def draw_resident_cache(key, part):
    level_set = key_amplitudes()
    filled = keyed_cache(key, SLOTS, 13, level_set)
    return filled.reshape(SLOTS, BLOCK_LEN, -1, KV_HEADS, 2 * HEAD_DIM).astype(jnp.bfloat16)


def draw_queries(key, part):
    group_size = HEADS // KV_HEADS
    direction = sign_direction(key)
    head_dirs = jnp.repeat(direction, group_size, axis=0)
    mask_key, level_key, noise_key, fine_key = jax.random.split(jax.random.fold_in(key, 17), 4)
    drawn = jnp.clip(jax.random.normal(noise_key, (SLOTS, HEADS, HEAD_DIM), jnp.float32), -6.0, 6.0)
    picked = jax.random.bernoulli(mask_key, 0.25, (SLOTS, HEADS))
    strength = jax.random.uniform(level_key, (SLOTS, HEADS), jnp.float32, 2.2, 5.5)
    fine_noise = 0.1 * jnp.clip(jax.random.normal(fine_key, (SLOTS, HEADS, HEAD_DIM), jnp.float32), -3.0, 3.0)
    aligned = jnp.clip(strength[..., None] * head_dirs[None] + fine_noise, -6.0, 6.0)
    return jnp.where(picked[..., None], aligned, drawn).astype(jnp.bfloat16)


def set_ends(result, key, least, top_value):
    place = [jax.random.randint(jax.random.fold_in(key, axis), (), 0, length) for axis, length in enumerate(result.shape)]
    longest = result.shape.index(max(result.shape))
    neighbour = place[:longest] + [(place[longest] + 1) % result.shape[longest]] + place[longest + 1:]
    return result.at[tuple(place)].set(least).at[tuple(neighbour)].set(top_value)


def strengthened(drawn, own_key, source, target, parts, factor):
    def block_of(axis_at):
        return (jnp.arange(drawn.shape[axis_at]) // (drawn.shape[axis_at] // parts)).reshape((-1,) + (1,) * (drawn.ndim - 1 - axis_at))

    near = jax.random.permutation(own_key, parts)[block_of(target)]
    other_side = (block_of(target) + parts // 2) % parts
    return jnp.where((block_of(source) == near) | (block_of(source) == other_side), factor * drawn, drawn)


def block_scale(stream_key, extent, pieces, least, top_value):
    def one(dim, parts):
        draws = jax.random.uniform(jax.random.fold_in(jax.random.fold_in(stream_key, 6), dim), (parts,), jnp.float32, least / len(pieces), top_value / len(pieces))
        return jnp.repeat(jnp.exp(draws), extent[dim] // parts).reshape((-1,) + (1,) * (len(extent) - dim - 1))

    level = one(*pieces[0])
    for cut in pieces[1:]:
        level = level * one(*cut)
    return level


def gaussian(key, extent, width, reach, shards=(), held_as=jnp.bfloat16):
    drawn = jax.random.normal(key, extent, jnp.float32) * width
    if len(shards) > 0:
        drawn = block_scale(key, extent, shards, -0.22, 0.18) * drawn
    return jnp.clip(drawn, min=-reach, max=reach).astype(held_as)


def heavy_noise(own_key, extent, spread, bound, cuts, heavy, held_as=jnp.bfloat16):
    values = spread * jax.random.normal(own_key, extent, jnp.float32)
    if cuts:
        values = values * block_scale(own_key, extent, cuts, -0.22, 0.18)
    return jnp.clip(strengthened(values, jax.random.fold_in(own_key, 3), *heavy), -bound, bound).astype(held_as)


def setup_inputs(seed: int = 0, part: int = 0) -> dict:
    key_list = jax.random.split(jax.random.key(seed), 18)
    part_keys = jax.random.split(jax.random.fold_in(key_list[17], part), 18)
    prompt_cache = draw_prompt_cache(jax.random.fold_in(jax.random.fold_in(key_list[17], part), 71), part)
    prompt_states = heavy_noise(part_keys[1], (PROMPTS, N_SEQ, STATE, INNER), 1.0, 6.0, ((0, 2), (1, 8)), (1, 3, 8, 2.0), jnp.float32)
    block_steps = jnp.clip(jnp.exp(math.log(0.1) - 2.9957323 * jax.random.uniform(part_keys[2], (PROMPTS, N_SEQ, INNER), jnp.float32) ** block_scale(part_keys[2], (PROMPTS, N_SEQ, INNER), ((0, 2), (1, 8)), -0.2, 0.2)), 0.005, 0.1)
    prompt_lengths = set_ends(jax.random.randint(part_keys[3], (PROMPTS,), PROMPT_MAX // 6, PROMPT_MAX), jax.random.fold_in(part_keys[3], 1), PROMPT_MAX // 6, PROMPT_MAX - 1).astype(jnp.int32)
    target_slots = draw_target_slots(jax.random.fold_in(jax.random.fold_in(key_list[17], part), 71), part)
    cache_lengths = set_ends(jax.random.randint(part_keys[5], (SLOTS,), PROMPT_MAX // 6, PROMPT_MAX), jax.random.fold_in(part_keys[5], 1), PROMPT_MAX // 6, PROMPT_MAX - 1).astype(jnp.int32)
    resident_cache = draw_resident_cache(jax.random.fold_in(jax.random.fold_in(key_list[17], part), 71), part)
    token_cache = gaussian(part_keys[7], (SLOTS, KV_HEADS, 2 * HEAD_DIM), 1.0, 6.0, ((0, 2),))
    queries = draw_queries(jax.random.fold_in(jax.random.fold_in(key_list[17], part), 71), part)
    resident_states = gaussian(part_keys[9], (SLOTS, STATE, INNER), 1.0, 6.0, ((0, 2), (2, 8)), jnp.float32)
    decay_rates = jnp.clip(jnp.exp(jax.random.uniform(key_list[10], (STATE, INNER), jnp.float32, math.log(0.05), math.log(10.0))), 0.05, 10.0)
    step_sizes = jnp.clip(jnp.exp(math.log(1.0) - 4.6051702 * jax.random.uniform(part_keys[11], (SLOTS, INNER), jnp.float32) ** block_scale(part_keys[11], (SLOTS, INNER), ((0, 2), (1, 8)), -0.2, 0.2)), 0.01, 1.0)
    inner_input = gaussian(part_keys[12], (SLOTS, INNER), 1.0, 6.0, ((0, 2), (1, 8)))
    inner_gate = gaussian(part_keys[13], (SLOTS, INNER), 1.0, 6.0, ((0, 2), (1, 8)))
    state_input = gaussian(part_keys[14], (SLOTS, STATE), 1.0, 6.0, ((0, 2),), jnp.float32)
    state_readout = gaussian(part_keys[15], (SLOTS, STATE), 1.0, 6.0, ((0, 2),), jnp.float32)
    skip_gain = jnp.clip(0.5 + 1.0 * jax.random.uniform(key_list[16], (INNER,), jnp.float32) ** block_scale(key_list[16], (INNER,), ((0, 8),), -0.2, 0.2), 0.5, 1.5)
    return {"prompt_cache": prompt_cache, "prompt_states": prompt_states, "block_steps": block_steps, "prompt_lengths": prompt_lengths, "target_slots": target_slots, "cache_lengths": cache_lengths, "resident_cache": resident_cache, "token_cache": token_cache, "queries": queries, "resident_states": resident_states, "decay_rates": decay_rates, "step_sizes": step_sizes, "inner_input": inner_input, "inner_gate": inner_gate, "state_input": state_input, "state_readout": state_readout, "skip_gain": skip_gain}


def reference(prompt_cache, prompt_states, block_steps, prompt_lengths, target_slots, cache_lengths, resident_cache, token_cache, queries, resident_states, decay_rates, step_sizes, inner_input, inner_gate, state_input, state_readout, skip_gain):
    prompt_max = BLOCK_LEN * N_SEQ
    slot_count = SLOTS_DEV * N_BATCH
    kv_width = 2 * HEAD_DIM
    slot_ids = jnp.arange(slot_count, dtype=jnp.int32)
    matches = target_slots[None, :] == slot_ids[:, None]
    fresh = jnp.any(matches, axis=1)
    chosen_len = lax.optimization_barrier(jnp.sum(jnp.where(matches, prompt_lengths[None, :], 0), axis=1)).astype(jnp.int32)
    lengths = jnp.where(fresh, chosen_len, cache_lengths).astype(jnp.int32)
    picked = jnp.dot(matches.astype(jnp.bfloat16), prompt_cache.reshape(PROMPTS, -1), preferred_element_type=jnp.float32)
    picked = picked.astype(jnp.bfloat16).reshape(slot_count, prompt_max, KV_HEADS, kv_width)
    resident = resident_cache.reshape(slot_count, prompt_max, KV_HEADS, kv_width)
    position = jnp.arange(prompt_max, dtype=jnp.int32)
    merged = jnp.where(fresh[:, None, None, None], picked, resident)
    merged = jnp.where((position[None, :] < lengths[:, None])[:, :, None, None], merged, jnp.zeros((), jnp.bfloat16))
    merged = jnp.where((position[None, :] == lengths[:, None])[:, :, None, None], token_cache[:, None], merged)
    merged_cache = merged.reshape(slot_count, BLOCK_LEN, N_SEQ, KV_HEADS, kv_width)
    group = HEADS // KV_HEADS
    grouped = queries.reshape(slot_count, KV_HEADS, group, HEAD_DIM).astype(jnp.float32)
    scores = jnp.einsum('rgqd,rtgd->rgqt', grouped, merged[..., :HEAD_DIM].astype(jnp.float32)) * (1.0 / math.sqrt(HEAD_DIM))
    seen = (position[None, :] <= lengths[:, None])[:, None, None, :]
    masked = jnp.where(seen, scores, -1e+30)
    masked = masked.reshape(slot_count, KV_HEADS, group, BLOCK_LEN, N_SEQ)
    seen_cls = jnp.broadcast_to(seen, scores.shape).reshape(slot_count, KV_HEADS, group, BLOCK_LEN, N_SEQ)
    class_top = lax.optimization_barrier(jnp.max(masked, axis=3))
    weights = jnp.where(seen_cls, jnp.exp(masked - class_top[:, :, :, None, :]), 0.0)
    class_total = lax.optimization_barrier(jnp.sum(weights, axis=3))
    values = merged_cache[..., HEAD_DIM:].astype(jnp.float32)
    class_sum = jnp.einsum('rgqij,rijgd->rgqjd', weights.astype(jnp.bfloat16).astype(jnp.float32), values)
    overall = lax.optimization_barrier(jnp.max(class_top, axis=3))
    factor = jnp.exp(class_top - overall[..., None])
    total = lax.optimization_barrier(jnp.sum(class_total * factor, axis=3))
    summed = lax.optimization_barrier(jnp.sum(class_sum * factor[..., None], axis=3))
    attention = (summed / total[..., None]).reshape(slot_count, HEADS, HEAD_DIM).astype(jnp.bfloat16)
    starts = jnp.arange(N_SEQ, dtype=jnp.int32) * BLOCK_LEN
    usable = (starts[None, :] < prompt_lengths[:, None]).astype(jnp.float32)
    step_terms = block_steps * usable[:, :, None]
    later = lax.optimization_barrier(jnp.sum(step_terms, axis=1, keepdims=True)) - jnp.cumsum(step_terms, axis=1)

    def fold_prompt(packed):
        states, behind, weight = packed
        return lax.optimization_barrier(jnp.sum(weight[:, None, None] * jnp.exp(-decay_rates[None] * behind[:, None, :]) * states, axis=0))
    handed = lax.map(fold_prompt, (prompt_states, later, usable))
    chosen_state = jnp.einsum('rp,pnc->rnc', matches.astype(jnp.float32), handed, precision=lax.Precision.HIGHEST)
    start = jnp.where(fresh[:, None, None], chosen_state, resident_states)
    inner = inner_input.astype(jnp.float32)
    next_states = jnp.exp(-decay_rates[None] * step_sizes[:, None, :]) * start + (step_sizes * inner)[:, None, :] * state_input[:, :, None]
    readout = lax.optimization_barrier(jnp.sum(state_readout[:, :, None] * next_states, axis=1)) + skip_gain[None, :] * inner
    mamba_output = (readout * jax.nn.silu(inner_gate.astype(jnp.float32))).astype(jnp.bfloat16)
    return (merged_cache, attention, next_states, mamba_output)
```

```python
import functools
import math

import jax
import jax.numpy as jnp
from jax import lax
from jax.experimental import pallas as pl
from jax.experimental.pallas import tpu as pltpu
from jax.sharding import PartitionSpec as P

MESH = pl.DeviceIdType.MESH
FULL = 32760.0
LOW = -1e30
PIECES = 4
LATE = 3
STEP_UNIT = float(1 << 18)
D_TIME, D_GAP = 3.6, 4.5
RELAY_TIME, ATTEND_TIME, ATTEND_GAP = 11.5, 13.0, 1.4
FOLD_TIME, FOLD_GAP, LEVEL_GAP = 10.4, 1.4, 6.0
LATE_TIME, LATE_GAP, LAST_GAP = 15.0, 4.5, 2.0


def to_int16(value):
    return jnp.round(value).astype(jnp.int32).astype(jnp.int16)


def to_float(value):
    return value.astype(jnp.int32).astype(jnp.float32)


def tile_lanes(row, width):
    return jnp.concatenate([row] * (width // 128), axis=1)


def lane_top(values):
    top = jnp.abs(values[0])
    for value in values[1:]:
        top = jnp.maximum(top, jnp.abs(value))
    parts = [top[:, i : i + 128] for i in range(0, top.shape[1], 128)]
    top = parts[0]
    for part in parts[1:]:
        top = jnp.maximum(top, part)
    return jnp.maximum(jnp.max(top, axis=0, keepdims=True), 1e-30)


def split_rows(value, size, bit):
    count = value.shape[0] // size
    even = [value[k * size : (k + 1) * size] for k in range(0, count, 2)]
    odd = [value[k * size : (k + 1) * size] for k in range(1, count, 2)]
    even = jnp.concatenate(even, axis=0) if len(even) > 1 else even[0]
    odd = jnp.concatenate(odd, axis=0) if len(odd) > 1 else odd[0]
    right = jnp.full(even.shape, bit, jnp.int32) == 1
    return jnp.where(right, odd, even), jnp.where(right, even, odd)


def pick(r, b, requests, all_prompts, plen, tslot, clen):
    slot = b * requests + r
    chosen, length, hits = jnp.int32(0), jnp.int32(0), jnp.int32(0)
    for p in range(all_prompts):
        hit = tslot[p] == slot
        chosen = jnp.where(hit, p, chosen)
        length = jnp.where(hit, plen[p], length)
        hits = jnp.where(hit, 1, hits)
    return chosen, hits, jnp.where(hits > 0, length, clen[r])


def exchange(dims, *refs):
    n, nb, levels, block_len, late_units = dims
    refs = list(refs)

    def take(count):
        out = refs[:count]
        del refs[:count]
        return out

    scalar_hbm = take(3)
    cache_hbm, states_hbm, steps_hbm, resident_hbm, token_hbm, queries_hbm, rates_hbm = take(7)
    through_hbm = take(7)
    merged, handed, orecv, lse_recv, rates_own = take(5)
    through = take(7)
    arrived, cache_send, states, steps, resident, token, queries, rates, osend, lse_all, lse_send = take(11)
    plen, tslot, clen = scalars = take(3)
    load_sems, state_sems, piece_sems, through_sems = take(4)
    d_send, d_recv, d_sel = take(levels), take(levels), take(levels)
    d_keep = take(levels - 1)
    q_send, q_recv = take(levels), take(levels)
    acc = take(levels - 1)
    m_send, m_recv = take(2)
    if late_units:
        zm_send, zm_recv, zsteps_send, zsteps_recv, zpre, zbuf = take(6)
        zd_send, zd_recv, zd_sel, zd_keep = (take(levels - 1) for _ in range(4))
        zd_ss, zd_rs, zm_ss, zm_rs = take(4)
    (
        cache_ss, cache_rs, relay_ss, relay_rs, d_ss, d_rs, q_ss, q_rs, m_ss, m_rs,
        hand_ss, hand_rs, o_ss, o_rs, l_ss, l_rs,
    ) = refs

    me = lax.axis_index("seq")
    b = lax.axis_index("batch")
    prompts, rows, _, kv_heads, width = cache_hbm.shape
    all_prompts = prompts * nb
    requests, heads, head_dim = queries.shape
    state_n, channels = rates.shape
    share_len = channels // n
    piece = share_len // PIECES
    own_heads = heads // n
    group = heads // kv_heads
    positions = resident.shape[1]
    bits = [lax.rem(me // (1 << s), 2) for s in range(levels)]
    peers = [me + (1 - 2 * bits[s]) * (1 << s) for s in range(levels)]
    first = b * prompts

    barrier = pltpu.get_barrier_semaphore()
    for k in range(1, n):
        pl.semaphore_signal(barrier, inc=1, device_id={"seq": lax.rem(me + k, n)}, device_id_type=MESH)
    for k in range(1, nb):
        pl.semaphore_signal(barrier, inc=1, device_id={"batch": lax.rem(b + k, nb)}, device_id_type=MESH)

    def load(src, dst, sem):
        copy = pltpu.make_async_copy(src, dst, sem)
        copy.start()
        return copy

    load_scalars = [load(src, dst, load_sems.at[6 + i]) for i, (src, dst) in enumerate(zip(scalar_hbm, scalars))]
    load_steps = load(steps_hbm, steps, load_sems.at[0])
    load_pieces = []
    for k in list(range(1, n)) + [0]:
        to = lax.rem(me + k, n)
        dst = cache_send.at[to] if k else arrived.at[b, me]
        load_pieces.append(load(cache_hbm.at[:, :, to], dst, piece_sems.at[k]))
    load_states = [load(states_hbm.at[0], states.at[0], state_sems.at[0])]
    load_rates = load(rates_hbm, rates, load_sems.at[1])
    for p in range(1, prompts):
        load_states.append(load(states_hbm.at[p], states.at[p], state_sems.at[p]))
    load_attention = [
        load(resident_hbm, resident, load_sems.at[2]),
        load(token_hbm, token, load_sems.at[3]),
        load(queries_hbm, queries, load_sems.at[4]),
    ]
    own_lanes = pl.ds(pl.multiple_of(me * share_len, 128), share_len)
    load_through = [load(rates_hbm.at[:, own_lanes], rates_own, load_sems.at[5])]
    for i, (src, dst) in enumerate(zip(through_hbm, through)):
        load_through.append(load(src, dst, through_sems.at[i]))

    def remote(src, dst, ss, rs, where):
        return pltpu.make_async_remote_copy(
            src_ref=src, dst_ref=dst, send_sem=ss, recv_sem=rs, device_id=where, device_id_type=MESH
        )

    def start(copy):
        copy.start()
        return copy

    def settle(ref, sem):
        pltpu.make_async_copy(ref, ref, sem).wait()

    def lanes(share, h):
        return pl.ds(pl.multiple_of(share * share_len + h * piece, 128), piece)

    for copy in load_scalars:
        copy.wait()
    usable = [
        jnp.where(me * block_len < plen[first + p], 1.0, 0.0).astype(jnp.float32)
        for p in range(prompts)
    ]

    pl.semaphore_wait(barrier, n - 1 + nb - 1)

    def send_cache(k):
        to = lax.rem(me + k, n)
        load_pieces[k - 1].wait()
        start(remote(cache_send.at[to], arrived.at[b, me], cache_ss.at[0], cache_rs.at[0], {"seq": to}))

    for k in range(2, n, 2):
        send_cache(k)

    step_width = min(512, share_len)
    row_id = lax.broadcasted_iota(jnp.int32, (prompts, step_width), 0)
    usable_rows = jnp.zeros((prompts, step_width), jnp.float32)
    for p in range(prompts):
        usable_rows = jnp.where(row_id == p, usable[p], usable_rows)

    def step_rows(bit, c):
        parts = []
        for k in range(n // 2):
            at = pl.ds(pl.multiple_of((2 * k + bit) * share_len + c * step_width, 128), step_width)
            parts.append(jnp.concatenate([steps[p, :, at] for p in range(prompts)], axis=0) * usable_rows)
        return jnp.concatenate(parts, axis=0)

    def columns(c):
        return pl.ds(pl.multiple_of(c * step_width, 128), step_width)

    m_copies = [
        remote(m_send.at[s], m_recv.at[s], m_ss.at[s], m_rs.at[s], {"seq": peers[s]}) for s in range(levels)
    ]
    d_copies = [
        remote(d_send[s], d_recv[s], d_ss.at[s], d_rs.at[s], {"seq": peers[s]}) for s in range(levels)
    ]
    load_steps.wait()

    @pl.loop(0, share_len // step_width)
    def _(c):
        d_send[0][:, columns(c)] = to_int16(step_rows(1 - bits[0], c) * STEP_UNIT)

    start(d_copies[0])

    def fold_steps(s):
        d_copies[s].wait_recv()

        @pl.loop(0, share_len // step_width)
        def _(c):
            at = columns(c)
            other = to_float(d_recv[s][:, at]) * ((1 << s) / STEP_UNIT)
            own = step_rows(bits[0], c) if s == 0 else d_keep[s - 1][:, at]
            selected = jnp.where(jnp.full(own.shape, bits[s], jnp.int32) == 1, own, other)
            for k in range(n >> (s + 1)):
                d_sel[s][k, :, at] = selected[k * prompts : (k + 1) * prompts]
            if s + 1 < levels:
                keep, send = split_rows(own + other, prompts, bits[s + 1])
                d_keep[s][:, at] = keep
                d_send[s + 1][:, at] = to_int16(send * (STEP_UNIT / (1 << (s + 1))))

        m_copies[s].wait_recv()
        if s + 1 < levels:
            start(d_copies[s + 1])
            m_send[s + 1] = m_send[s] + m_recv[s]
            start(m_copies[s + 1])

    half = n // 2
    late_bits = bits[1:] + bits[:1]
    late_peers = peers[1:] + peers[:1]
    late_me = me // 2 + lax.rem(me, 2) * half
    units = [(p, h) for p in range(prompts) for h in range(PIECES)]
    total_units = len(units)
    plain = list(range(total_units - late_units))
    late = list(range(total_units - late_units, total_units))
    late_prompt = prompts - 1
    late_from = PIECES - late_units

    def is_late(u):
        return u >= total_units - late_units

    def bit_of(s, u):
        return late_bits[s] if is_late(u) else bits[s]

    def late_share(v):
        return lax.rem(v, half) * 2 + v // half

    q_copies = {}

    def send_values(s, u, values, factor):
        bound = zm_send[s] if is_late(u) else m_send[s, units[u][0] : units[u][0] + 1]
        scale = tile_lanes(FULL / bound * factor, piece)
        for k, value in enumerate(values):
            q_send[s][u, k] = to_int16(value * scale)
        where = {"seq": (late_peers if is_late(u) else peers)[s]}
        q_copies[s, u] = start(remote(q_send[s].at[u], q_recv[s].at[u], q_ss.at[s], q_rs.at[s, u], where))

    def read(s, u, k):
        p, h = units[u]
        if s > 0:
            return acc[s - 1][u, k]
        if is_late(u):
            return zbuf[h - late_from, 2 * k + late_bits[0]]
        return states[p, :, lanes(2 * k + bits[0], h)] * usable[p]

    def first_send(u):
        p, h = units[u]
        if is_late(u):
            values = [zbuf[h - late_from, 2 * k + 1 - late_bits[0]] for k in range(half)]
            send_values(0, u, values, 1.0)
        else:
            values = [states[p, :, lanes(2 * k + 1 - bits[0], h)] for k in range(half)]
            send_values(0, u, values, usable[p])

    def fold(s, u):
        p, h = units[u]
        q_copies[s, u].wait_recv()
        bound = zm_recv[s] if is_late(u) else m_recv[s, p : p + 1]
        scale = tile_lanes(bound * (1.0 / FULL), piece)
        right = jnp.full((state_n, piece), bit_of(s, u), jnp.int32) == 1
        below = lax.rem(late_me if is_late(u) else me, 1 << (s + 1))

        def folded(k):
            other = to_float(q_recv[s][u, k]) * scale
            own = read(s, u, k)
            if is_late(u) and s == levels - 1:
                return own + other
            v = k * (1 << (s + 1)) + below
            if is_late(u):
                share = late_share(v)
                late_at = (h - late_from) * piece
                behind = zd_sel[s][k][:, late_at : late_at + piece]
            else:
                share = v
                behind = d_sel[s][k, p : p + 1, h * piece : (h + 1) * piece]
            decay = jnp.exp(-rates[:, lanes(share, h)] * behind)
            early = jnp.where(right, other, own)
            later = jnp.where(right, own, other)
            return decay * early + later

        if s + 1 < levels:
            bit = bit_of(s + 1, u)
            count = n >> (s + 2)
            send_values(s + 1, u, [folded(2 * k + 1 - bit) for k in range(count)], 1.0)
            for k in range(count):
                acc[s][u, k] = folded(2 * k + bit)
        else:
            at = pl.ds(h * piece, piece)
            handed[first + p, :, at] = folded(0)
            for k in range(1, nb):
                start(
                    remote(
                        handed.at[first + p, :, at],
                        handed.at[first + p, :, at],
                        hand_ss.at[k - 1],
                        hand_rs.at[k - 1],
                        {"batch": lax.rem(b + k, nb)},
                    )
                )

    if late_units:
        late_lanes = late_units * piece

        def late_row(v):
            at = ((v % half) * 2 + v // half) * share_len + late_from * piece
            return steps[late_prompt, :, at : at + late_lanes]

        def late_rows():
            return jnp.concatenate([late_row(v) for v in range(n)], axis=0) * usable[late_prompt]

        zd_copies = [remote(zsteps_send, zsteps_recv, zd_ss.at[0], zd_rs.at[0], {"seq": peers[0]})]
        for i in range(levels - 1):
            zd_copies.append(
                remote(zd_send[i], zd_recv[i], zd_ss.at[i + 1], zd_rs.at[i + 1], {"seq": late_peers[i]})
            )
        zm_copies = [
            remote(zm_send.at[s], zm_recv.at[s], zm_ss.at[s], zm_rs.at[s], {"seq": late_peers[s]})
            for s in range(levels)
        ]
        zsteps_send[...] = to_int16(late_rows() * STEP_UNIT)
        start(zd_copies[0])

        def late_split(i, value):
            keep, send = split_rows(value, 1, late_bits[i])
            zd_keep[i][...] = keep
            zd_send[i][...] = send
            start(zd_copies[i + 1])

        def late_begin():
            zd_copies[0].wait_recv()
            other = to_float(zsteps_recv[...]) * (1.0 / STEP_UNIT)
            before = jnp.where(jnp.full(other.shape, bits[0], jnp.int32) == 1, 0.0, other)
            for v in range(n):
                zpre[v] = before[v : v + 1]
            late_split(0, late_rows() + other)

            @pl.loop(0, n)
            def _(v):
                row = zpre[v]
                for i in range(late_units):
                    at = lanes(late_share(v), late_from + i)
                    decay = jnp.exp(-rates[:, at] * row[:, i * piece : (i + 1) * piece])
                    zbuf[i, v] = states[late_prompt, :, at] * decay * usable[late_prompt]

            zm_send[0] = m_send[0, late_prompt : late_prompt + 1]
            start(zm_copies[0])
            for u in late:
                first_send(u)

        def late_steps(i):
            zd_copies[i + 1].wait_recv()
            zm_copies[i].wait_recv()
            zm_send[i + 1] = zm_send[i] + zm_recv[i]
            start(zm_copies[i + 1])
            own, other = zd_keep[i][...], zd_recv[i][...]
            selected = jnp.where(jnp.full(own.shape, late_bits[i], jnp.int32) == 1, own, other)
            for k in range(n >> (i + 1)):
                zd_sel[i][k] = selected[k : k + 1]
            if i + 1 < levels - 1:
                late_split(i + 1, own + other)

    for k in range(1, n, 2):
        send_cache(k)
    load_pieces[n - 1].wait()

    relays = [
        remote(
            arrived.at[b], arrived.at[b], relay_ss.at[k - 1], relay_rs.at[k - 1], {"batch": lax.rem(b + k, nb)}
        )
        for k in range(1, nb)
    ]

    top_width = min(512, share_len)
    for p in range(prompts):
        load_states[p].wait()

        def larger(i, top):
            at = pl.ds(pl.multiple_of(i * top_width, 128), top_width)
            return jnp.maximum(top, jnp.abs(states[p, :, at]))

        top = lax.fori_loop(0, channels // top_width, larger, jnp.zeros((state_n, top_width), jnp.float32), unroll=4)
        m_send[0, p : p + 1] = jnp.maximum(lane_top([top]) * usable[p], 1e-30)
    start(m_copies[0])
    for u in plain:
        first_send(u)

    shape3 = (positions, kv_heads, width)
    position = lax.broadcasted_iota(jnp.int32, shape3, 0) * n + me
    flat = positions * kv_heads
    column = lax.broadcasted_iota(jnp.int32, (heads, flat), 1)
    owner = lax.broadcasted_iota(jnp.int32, (heads, flat), 0) // group
    same_head = lax.rem(column, kv_heads) == owner
    column_position = (column // kv_heads) * n + me
    lane_id = lax.broadcasted_iota(jnp.int32, (heads, 128), 1)

    def attend(r):
        chosen, hits, length = pick(r, b, requests, all_prompts, plen, tslot, clen)
        fresh_limit = jnp.where(hits > 0, length, 0)
        new = arrived[chosen // prompts, :, lax.rem(chosen, prompts)].reshape(shape3).astype(jnp.float32)
        old = resident[r].astype(jnp.float32)
        x = jnp.where(position < fresh_limit, new, old)
        x = jnp.where(position < length, x, 0.0)
        x = jnp.where(position == length, token[r].astype(jnp.float32)[None], x)
        merged[r] = x.astype(jnp.bfloat16)
        x2 = x.reshape(flat, width)
        keys = x2[:, :head_dim].astype(jnp.bfloat16)
        values = x2[:, head_dim:].astype(jnp.bfloat16)
        score = lax.dot_general(
            queries[r], keys, (((1,), (1,)), ((), ())), preferred_element_type=jnp.float32
        ) * (1.0 / math.sqrt(head_dim))
        seen = same_head & (column_position <= length)
        score = jnp.where(seen, score, LOW)
        top = jnp.max(score, axis=1, keepdims=True)
        weight = jnp.where(seen, jnp.exp(score - top), 0.0)
        total = jnp.sum(weight, axis=1, keepdims=True)
        out = jnp.dot(weight.astype(jnp.bfloat16), values, preferred_element_type=jnp.float32)
        some = total > 0.0
        safe = jnp.where(some, total, 1.0)
        out = out / safe
        lse = jnp.where(some, top + jnp.log(safe), LOW)
        peak = jnp.maximum(jnp.max(jnp.abs(out), axis=1, keepdims=True), 1e-30)
        coded = jnp.round(out * (FULL / peak)).astype(jnp.int32)
        for j in range(n):
            osend[j, r * own_heads : (r + 1) * own_heads] = coded[j * own_heads : (j + 1) * own_heads].astype(jnp.int16)
        noted = jnp.where(lane_id == r, lse, lse_all[...])
        lse_all[...] = jnp.where(lane_id == requests + r, peak * (1.0 / FULL), noted)

    def attention_begin():
        settle(arrived.at[b, pl.ds(0, n - 1)], cache_rs.at[0])
        for copy in relays:
            start(copy)
        for copy in load_attention:
            copy.wait()
        lse_all[...] = jnp.zeros((heads, 128), jnp.float32)

    def attention_end():
        for j in range(n):
            lse_send[j] = lse_all[j * own_heads : (j + 1) * own_heads]
        for k in range(1, n):
            to = lax.rem(me + k, n)
            start(remote(lse_send.at[to], lse_recv.at[me], l_ss.at[0], l_rs.at[0], {"seq": to}))
            start(remote(osend.at[to], orecv.at[me], o_ss.at[0], o_rs.at[0], {"seq": to}))
        lse_recv[me] = lse_send[me]
        orecv[me] = osend[me]

    load_rates.wait()

    def attend_some(r):
        if r == 0:
            for copy in relays:
                copy.wait_recv()
        attend(r)
        if r == requests - 1:
            attention_end()

    def fold_late(s):
        if s == levels - 1:
            zm_copies[s].wait_recv()
        for u in late:
            fold(s, u)

    events = [(D_TIME + D_GAP * s, functools.partial(fold_steps, s)) for s in range(levels)]
    events.append((RELAY_TIME, attention_begin))
    events += [(ATTEND_TIME + ATTEND_GAP * r, functools.partial(attend_some, r)) for r in range(requests)]
    for i, u in enumerate(plain):
        for s in range(levels):
            events.append((FOLD_TIME + FOLD_GAP * i + LEVEL_GAP * s, functools.partial(fold, s, u)))
    if late_units:
        events.append((D_TIME + 0.1, late_begin))
        for s in range(1, levels):
            events.append((D_TIME + D_GAP * s + 0.1, functools.partial(late_steps, s - 1)))
            events.append((LATE_TIME + LATE_GAP * (s - 1), functools.partial(fold_late, s - 1)))
        last = FOLD_TIME + FOLD_GAP * len(plain) + LAST_GAP
        events.append((last, functools.partial(fold_late, levels - 1)))
    for _, event in sorted(events, key=lambda e: e[0]):
        event()

    for copy in load_through:
        copy.wait()
    others = pl.ds(0, n - 1)
    settle(lse_recv.at[others], l_rs.at[0])
    settle(orecv.at[others], o_rs.at[0])
    for k in range(1, nb):
        theirs = pl.ds(lax.rem(b + nb - k, nb) * prompts, prompts)
        settle(handed.at[theirs], hand_rs.at[k - 1])
        settle(handed.at[pl.ds(first, prompts)], hand_ss.at[k - 1])
    settle(cache_send.at[others], cache_ss.at[0])
    settle(lse_send.at[others], l_ss.at[0])
    settle(osend.at[others], o_ss.at[0])
    for s in range(levels):
        settle(q_send[s], q_ss.at[s])
    for copy in relays + d_copies + m_copies + (zd_copies + zm_copies if late_units else []):
        copy.wait_send()


def finish(dims, plen, tslot, clen, merged, handed, orecv, lse_recv, rates, rstates, dt, inner, gate, s_in, s_out, skip,
           merged_out, attention_out, nstates_out, mout_out, nstates, mout, attention, sems):
    n, nb = dims
    b = lax.axis_index("batch")
    all_prompts = handed.shape[0]
    requests, state_n, share_len = rstates.shape
    own_heads, head_dim = attention.shape[1:]
    chunk = min(512, share_len)
    per_share = share_len // chunk

    copies = []

    def out(src, dst, i):
        copy = pltpu.make_async_copy(src, dst, sems.at[i])
        copy.start()
        copies.append(copy)

    out(merged, merged_out, 0)
    eye = lax.broadcasted_iota(jnp.int32, (state_n, state_n), 0) == lax.broadcasted_iota(
        jnp.int32, (state_n, state_n), 1
    )

    def as_column(row):
        spread = jnp.where(eye, jnp.broadcast_to(row, (state_n, state_n)), 0.0)
        return jnp.sum(spread, axis=1, keepdims=True)

    picks = [pick(r, b, requests, all_prompts, plen, tslot, clen) for r in range(requests)]
    in_all, out_all = s_in[...], s_out[...]
    in_cols = [as_column(in_all[r : r + 1]) for r in range(requests)]
    out_cols = [as_column(out_all[r : r + 1]) for r in range(requests)]

    for c in range(per_share):
        at = pl.ds(c * chunk, chunk)
        step_rows = dt[:, at]
        x_rows = inner[:, at].astype(jnp.float32)
        g = gate[:, at].astype(jnp.float32)
        rate = -rates[:, at]
        push_rows = step_rows * x_rows
        out_rows = []
        for r in range(requests):
            chosen, hits, _ = picks[r]
            fresh = jnp.full((state_n, chunk), hits, jnp.int32) > 0
            begin = jnp.where(fresh, handed[chosen, :, at], rstates[r, :, at])
            after = jnp.exp(rate * step_rows[r : r + 1]) * begin
            after = after + push_rows[r : r + 1] * in_cols[r]
            nstates[r, :, at] = after
            out_rows.append(jnp.sum(out_cols[r] * after, axis=0, keepdims=True))
        out(nstates.at[:, :, at], nstates_out.at[:, :, at], 3 + c)
        read_out = jnp.concatenate(out_rows, axis=0) + skip[:, at] * x_rows
        mout[:, at] = (read_out * (g / (1.0 + jnp.exp(-g)))).astype(jnp.bfloat16)
    out(mout, mout_out, 1)

    lane3 = lax.broadcasted_iota(jnp.int32, (n, own_heads, 128), 2)
    noted = lse_recv[...]
    for r in range(requests):
        lse = jnp.sum(jnp.where(lane3 == r, noted, 0.0), axis=2, keepdims=True)
        unit = jnp.sum(jnp.where(lane3 == requests + r, noted, 0.0), axis=2, keepdims=True)
        share = jnp.exp(lse - jnp.max(lse, axis=0, keepdims=True))
        parts = to_float(orecv[:, r * own_heads : (r + 1) * own_heads])
        top = jnp.sum(share * unit * parts, axis=0)
        attention[r] = (top / jnp.sum(share, axis=0)).astype(jnp.bfloat16)
    out(attention, attention_out, 2)
    for copy in copies:
        copy.wait()


def local(
    n,
    nb,
    prompt_cache,
    prompt_states,
    block_steps,
    prompt_lengths,
    target_slots,
    cache_lengths,
    resident_cache,
    token_cache,
    queries,
    resident_states,
    decay_rates,
    step_sizes,
    inner_input,
    inner_gate,
    state_input,
    state_readout,
    skip_gain,
):
    levels = n.bit_length() - 1
    prompts, block_len, kv_heads, width = prompt_cache.shape
    requests, heads, head_dim = queries.shape
    state_n, channels = decay_rates.shape
    share = channels // n
    piece = share // PIECES
    own_heads = heads // n
    positions = resident_cache.shape[1]
    all_prompts = prompts * nb
    rows = block_len // n
    unit_count = prompts * PIECES
    late_units = LATE
    f32, bf16, i16 = jnp.float32, jnp.bfloat16, jnp.int16
    vmem = pl.BlockSpec(memory_space=pltpu.VMEM)
    smem = pl.BlockSpec(memory_space=pltpu.SMEM)
    hbm = pl.BlockSpec(memory_space=pltpu.HBM)
    dma = pltpu.SemaphoreType.DMA
    halves = [n >> (s + 1) for s in range(levels)]
    through = (resident_states, step_sizes, inner_input, inner_gate, state_input, state_readout, skip_gain[None])
    operands = (
        prompt_cache.reshape(prompts, rows, n, kv_heads, width),
        prompt_states[:, 0],
        block_steps,
        resident_cache[:, :, 0],
        token_cache,
        queries,
        decay_rates,
    ) + through
    outs = (
        pltpu.VMEM((requests, positions, kv_heads, width), bf16),
        pltpu.VMEM((all_prompts, state_n, share), f32),
        pltpu.VMEM((n, requests * own_heads, head_dim), i16),
        pltpu.VMEM((n, own_heads, 128), f32),
        pltpu.VMEM((state_n, share), f32),
    ) + tuple(pltpu.VMEM(x.shape, x.dtype) for x in through)
    scratch = [
        pltpu.VMEM((nb, n, prompts, rows, kv_heads, width), bf16),
        pltpu.VMEM((n, prompts, rows, kv_heads, width), bf16),
        pltpu.VMEM((prompts, state_n, channels), f32),
        pltpu.VMEM(block_steps.shape, f32),
        pltpu.VMEM((requests, positions, kv_heads, width), bf16),
        pltpu.VMEM(token_cache.shape, bf16),
        pltpu.VMEM(queries.shape, bf16),
        pltpu.VMEM(decay_rates.shape, f32),
        pltpu.VMEM((n, requests * own_heads, head_dim), i16),
        pltpu.VMEM((heads, 128), f32),
        pltpu.VMEM((n, own_heads, 128), f32),
        pltpu.SMEM(prompt_lengths.shape, jnp.int32),
        pltpu.SMEM(target_slots.shape, jnp.int32),
        pltpu.SMEM(cache_lengths.shape, jnp.int32),
        dma((9,)),
        dma((prompts,)),
        dma((n,)),
        dma((len(through),)),
    ]
    for _ in range(2):
        scratch += [pltpu.VMEM((h * prompts, share), i16) for h in halves]
    scratch += [pltpu.VMEM((h, prompts, share), f32) for h in halves]
    scratch += [pltpu.VMEM((h * prompts, share), f32) for h in halves[1:]]
    for _ in range(2):
        scratch += [pltpu.VMEM((unit_count, h, state_n, piece), i16) for h in halves]
    scratch += [pltpu.VMEM((unit_count, h, state_n, piece), f32) for h in halves[1:]]
    scratch += [pltpu.VMEM((levels, prompts, 128), f32)] * 2
    if late_units:
        late_lanes = late_units * piece
        scratch += [pltpu.VMEM((levels, 1, 128), f32)] * 2
        scratch += [pltpu.VMEM((n, late_lanes), i16)] * 2
        scratch += [pltpu.VMEM((n, 1, late_lanes), f32)]
        scratch += [pltpu.VMEM((late_units, n, state_n, piece), f32)]
        for _ in range(2):
            scratch += [pltpu.VMEM((h, late_lanes), f32) for h in halves[: levels - 1]]
        scratch += [pltpu.VMEM((h, 1, late_lanes), f32) for h in halves[: levels - 1]]
        scratch += [pltpu.VMEM((h, late_lanes), f32) for h in halves[: levels - 1]]
        scratch += [dma((levels,))] * 4
    scratch += [dma((1,))] * 2
    scratch += [dma((max(nb - 1, 1),))] * 2
    scratch += [dma((levels,))] * 2
    scratch += [dma((levels,)), dma((levels, unit_count))]
    scratch += [dma((levels,))] * 2
    scratch += [dma((max(nb - 1, 1),))] * 2
    scratch += [dma((1,))] * 4
    scalars = [
        pltpu.with_memory_space_constraint(x, pltpu.HBM)
        for x in (prompt_lengths, target_slots, cache_lengths)
    ]
    parts = pl.pallas_call(
        functools.partial(exchange, (n, nb, levels, block_len, late_units)),
        out_shape=outs,
        in_specs=[hbm] * (3 + len(operands)),
        out_specs=(vmem,) * len(outs),
        scratch_shapes=scratch,
        compiler_params=pltpu.CompilerParams(
            collective_id=0, has_side_effects=True, vmem_limit_bytes=40 << 20
        ),
    )(*scalars, *(pltpu.with_memory_space_constraint(x, pltpu.HBM) for x in operands))
    chunks = share // min(512, share)
    merged, attention, next_states, mamba_output = pl.pallas_call(
        functools.partial(finish, (n, nb)),
        out_shape=(
            jax.ShapeDtypeStruct((requests, positions, kv_heads, width), bf16),
            jax.ShapeDtypeStruct((requests, own_heads, head_dim), bf16),
            jax.ShapeDtypeStruct((requests, state_n, share), f32),
            jax.ShapeDtypeStruct((requests, share), bf16),
        ),
        in_specs=[smem] * 3 + [vmem] * len(parts),
        out_specs=(hbm,) * 4,
        scratch_shapes=[
            pltpu.VMEM((requests, state_n, share), f32),
            pltpu.VMEM((requests, share), bf16),
            pltpu.VMEM((requests, own_heads, head_dim), bf16),
            dma((3 + chunks,)),
        ],
        compiler_params=pltpu.CompilerParams(vmem_limit_bytes=16 << 20),
    )(*scalars, *parts)
    return merged[:, :, None], attention, next_states, mamba_output


def solution(mesh):
    n, nb = mesh.shape["seq"], mesh.shape["batch"]
    return jax.shard_map(
        functools.partial(local, n, nb),
        mesh=mesh,
        in_specs=(
            P(("groups", "batch"), "seq", None, None),
            P(("groups", "batch"), "seq", None, None),
            P(("groups", "batch"), "seq", None),
            P("groups"),
            P("groups"),
            P(("groups", "batch")),
            P(("groups", "batch"), None, "seq", None, None),
            P(("groups", "batch"), None, None),
            P(("groups", "batch"), None, None),
            P(("groups", "batch"), None, "seq"),
            P(),
            P(("groups", "batch"), "seq"),
            P(("groups", "batch"), "seq"),
            P(("groups", "batch"), "seq"),
            P(("groups", "batch"), None),
            P(("groups", "batch"), None),
            P("seq"),
        ),
        out_specs=(
            P(("groups", "batch"), None, "seq", None, None),
            P(("groups", "batch"), "seq", None),
            P(("groups", "batch"), None, "seq"),
            P(("groups", "batch"), "seq"),
        ),
        check_vma=False,
    )
```

```python
import functools
import math

import jax
import jax.numpy as jnp
from jax import lax
from jax.experimental import pallas as pl
from jax.experimental.pallas import tpu as pltpu
from jax.sharding import PartitionSpec as P

MESH = pl.DeviceIdType.MESH
FULL = 32760.0
LOW = -1e30
PIECES = 4
LATE = 2
STEP_UNIT = float(1 << 18)
D_TIME, D_GAP = 4.5, 4.6
BOUND_TIME, BOUND_GAP = 6.5, 3.5
RELAY_TIME, ATTEND_TIME, ATTEND_GAP = 14.5, 15.5, 0.5
OUT_TIME, OUT_GAP = 19.5, 0.05
FOLD_TIME, FOLD_GAP, FIRST_LAG, NEXT_LAG = 8.8, 1.39, 5.5, 5.5
LATE_TIME, LATE_GAP, LAST_GAP = 16.0, 0.5, 4.0


def to_int16(value):
    return jnp.round(value).astype(jnp.int32).astype(jnp.int16)


def to_float(value):
    return value.astype(jnp.int32).astype(jnp.float32)


def tile_lanes(row, width):
    return jnp.concatenate([row] * (width // 128), axis=1)


def lane_top(values):
    top = jnp.abs(values[0])
    for value in values[1:]:
        top = jnp.maximum(top, jnp.abs(value))
    parts = [top[:, i : i + 128] for i in range(0, top.shape[1], 128)]
    top = parts[0]
    for part in parts[1:]:
        top = jnp.maximum(top, part)
    return jnp.maximum(jnp.max(top, axis=0, keepdims=True), 1e-30)


def split_rows(value, size, bit):
    count = value.shape[0] // size
    even = [value[k * size : (k + 1) * size] for k in range(0, count, 2)]
    odd = [value[k * size : (k + 1) * size] for k in range(1, count, 2)]
    even = jnp.concatenate(even, axis=0) if len(even) > 1 else even[0]
    odd = jnp.concatenate(odd, axis=0) if len(odd) > 1 else odd[0]
    right = jnp.full(even.shape, bit, jnp.int32) == 1
    return jnp.where(right, odd, even), jnp.where(right, even, odd)


def pick(r, b, requests, all_prompts, plen, tslot, clen):
    slot = b * requests + r
    chosen, length, hits = jnp.int32(0), jnp.int32(0), jnp.int32(0)
    for p in range(all_prompts):
        hit = tslot[p] == slot
        chosen = jnp.where(hit, p, chosen)
        length = jnp.where(hit, plen[p], length)
        hits = jnp.where(hit, 1, hits)
    return chosen, hits, jnp.where(hits > 0, length, clen[r])


def exchange(dims, *refs):
    n, nb, levels, block_len, late_units = dims
    refs = list(refs)

    def take(count):
        out = refs[:count]
        del refs[:count]
        return out

    scalar_hbm = take(3)
    cache_hbm, states_hbm, steps_hbm, resident_hbm, token_hbm, queries_hbm, rates_hbm = take(7)
    through_hbm = take(7)
    merged, handed, orecv, lse_recv, rates_own = take(5)
    through = take(7)
    arrived, states, steps, resident, token, queries, rates, osend, lse_all, lse_send = take(10)
    plen, tslot, clen = scalars = take(3)
    load_sems, state_sems, through_sems = take(3)
    d_send, d_recv, d_sel = take(levels), take(levels), take(levels)
    d_keep = take(levels - 1)
    q_send, q_recv = take(levels), take(levels)
    acc = take(levels - 1)
    table, bound_own, bound_peer = take(3)
    if late_units:
        late_own, late_peer, zsteps_send, zsteps_recv, zpre = take(5)
        zd_send, zd_recv, zd_sel, zd_keep = take(4)
        zd_ss, zd_rs = take(2)
    (
        cache_ss, cache_rs, relay_ss, relay_rs, d_ss, d_rs, q_ss, q_rs, m_ss, m_rs,
        hand_ss, hand_rs, o_ss, o_rs, l_ss, l_rs,
    ) = refs

    me = lax.axis_index("seq")
    b = lax.axis_index("batch")
    prompts, rows, _, kv_heads, width = cache_hbm.shape
    all_prompts = prompts * nb
    requests, heads, head_dim = queries.shape
    state_n, channels = rates.shape
    share_len = channels // n
    piece = share_len // PIECES
    own_heads = heads // n
    group = heads // kv_heads
    positions = resident.shape[1]
    bits = [lax.rem(me // (1 << s), 2) for s in range(levels)]
    peers = [me + (1 - 2 * bits[s]) * (1 << s) for s in range(levels)]
    first = b * prompts

    barrier = pltpu.get_barrier_semaphore()
    for k in range(1, n):
        pl.semaphore_signal(barrier, inc=1, device_id={"seq": lax.rem(me + k, n)}, device_id_type=MESH)
    for k in range(1, nb):
        pl.semaphore_signal(barrier, inc=1, device_id={"batch": lax.rem(b + k, nb)}, device_id_type=MESH)

    def load(src, dst, sem):
        copy = pltpu.make_async_copy(src, dst, sem)
        copy.start()
        return copy

    load_scalars = [load(src, dst, load_sems.at[6 + i]) for i, (src, dst) in enumerate(zip(scalar_hbm, scalars))]
    load_steps = load(steps_hbm, steps, load_sems.at[0])
    load_states = [load(states_hbm.at[0], states.at[0], state_sems.at[0])]
    load_piece = load(cache_hbm.at[:, :, me], arrived.at[b, me], load_sems.at[9])
    load_rates = load(rates_hbm, rates, load_sems.at[1])
    for p in range(1, prompts):
        load_states.append(load(states_hbm.at[p], states.at[p], state_sems.at[p]))
    load_attention = [
        load(resident_hbm, resident, load_sems.at[2]),
        load(token_hbm, token, load_sems.at[3]),
        load(queries_hbm, queries, load_sems.at[4]),
    ]
    own_lanes = pl.ds(pl.multiple_of(me * share_len, 128), share_len)
    load_through = [load(rates_hbm.at[:, own_lanes], rates_own, load_sems.at[5])]
    for i, (src, dst) in enumerate(zip(through_hbm, through)):
        load_through.append(load(src, dst, through_sems.at[i]))

    def remote(src, dst, ss, rs, where):
        return pltpu.make_async_remote_copy(
            src_ref=src, dst_ref=dst, send_sem=ss, recv_sem=rs, device_id=where, device_id_type=MESH
        )

    def start(copy):
        copy.start()
        return copy

    def settle(ref, sem):
        pltpu.make_async_copy(ref, ref, sem).wait()

    def lanes(share, h):
        return pl.ds(pl.multiple_of(share * share_len + h * piece, 128), piece)

    pl.semaphore_wait(barrier, n - 1 + nb - 1)

    def across(k):
        to = me
        for i in range(levels):
            if (k >> i) % 2:
                to = to + peers[i] - me
        return to

    def send_cache(k):
        to = across(k)
        start(remote(cache_hbm.at[:, :, to], arrived.at[b, me], cache_ss.at[0], cache_rs.at[0], {"seq": to}))

    for k in range(n - 1, 1, -2):
        send_cache(k)
    for k in range(n - 2, 0, -2):
        send_cache(k)

    for copy in load_scalars:
        copy.wait()
    usable = [
        jnp.where(me * block_len < plen[first + p], 1.0, 0.0).astype(jnp.float32)
        for p in range(prompts)
    ]

    step_width = min(512, share_len)
    row_id = lax.broadcasted_iota(jnp.int32, (prompts, step_width), 0)
    usable_rows = jnp.zeros((prompts, step_width), jnp.float32)
    for p in range(prompts):
        usable_rows = jnp.where(row_id == p, usable[p], usable_rows)

    def step_rows(bit, c):
        parts = []
        for k in range(n // 2):
            at = pl.ds(pl.multiple_of((2 * k + bit) * share_len + c * step_width, 128), step_width)
            parts.append(jnp.concatenate([steps[p, :, at] for p in range(prompts)], axis=0) * usable_rows)
        return jnp.concatenate(parts, axis=0)

    def columns(c):
        return pl.ds(pl.multiple_of(c * step_width, 128), step_width)

    d_copies = [
        remote(d_send[s], d_recv[s], d_ss.at[s], d_rs.at[s], {"seq": peers[s]}) for s in range(levels)
    ]
    load_steps.wait()

    @pl.loop(0, share_len // step_width)
    def _(c):
        d_send[0][:, columns(c)] = to_int16(step_rows(1 - bits[0], c) * STEP_UNIT)

    start(d_copies[0])

    def fold_steps(s):
        d_copies[s].wait_recv()

        @pl.loop(0, share_len // step_width)
        def _(c):
            at = columns(c)
            other = to_float(d_recv[s][:, at]) * ((1 << s) / STEP_UNIT)
            own = step_rows(bits[0], c) if s == 0 else d_keep[s - 1][:, at]
            selected = jnp.where(jnp.full(own.shape, bits[s], jnp.int32) == 1, own, other)
            for k in range(n >> (s + 1)):
                d_sel[s][k, :, at] = selected[k * prompts : (k + 1) * prompts]
            if s + 1 < levels:
                keep, send = split_rows(own + other, prompts, bits[s + 1])
                d_keep[s][:, at] = keep
                d_send[s + 1][:, at] = to_int16(send * (STEP_UNIT / (1 << (s + 1))))

        if s + 1 < levels:
            start(d_copies[s + 1])

    def bottom(device, s):
        return device - lax.rem(device, 1 << s)

    def fold_bounds(s):
        settle(table.at[pl.ds(0, 1 << s)], m_rs.at[s])

        def group_bound(device):
            total = table[bottom(device, s)]
            for i in range(1, 1 << s):
                total = total + table[bottom(device, s) + i]
            return total

        bound_peer[s] = group_bound(peers[s])
        if s + 1 < levels:
            bound_own[s + 1] = bound_own[s] + bound_peer[s]
        if late_units and s == 1:
            at = slice(late_prompt, late_prompt + 1)
            late_own[1] = table[me, at] + table[peers[1], at]
            late_peer[0] = table[peers[1], at]
            late_peer[1] = table[peers[0], at] + table[peers[0] + peers[1] - me, at]

    half = n // 2
    late_bits = [bits[1], bits[0]] + bits[2:]
    late_peers = [peers[1], peers[0]] + peers[2:]
    units = [(p, h) for p in range(prompts) for h in range(PIECES)]
    total_units = len(units)
    plain = list(range(total_units - late_units))
    late = list(range(total_units - late_units, total_units))
    late_prompt = prompts - 1
    late_from = PIECES - late_units

    def is_late(u):
        return u >= total_units - late_units

    def bit_of(s, u):
        return late_bits[s] if is_late(u) else bits[s]

    def late_share(v):
        return (v // 4) * 4 + (v % 2) * 2 + (v // 2) % 2

    q_copies = {}

    def send_values(s, u, values, factor):
        bound = late_own[s] if is_late(u) and s < 2 else bound_own[s, units[u][0] : units[u][0] + 1]
        scale = tile_lanes(FULL / bound * factor, piece)
        for k, value in enumerate(values):
            q_send[s][u, k] = to_int16(value * scale)
        where = {"seq": (late_peers if is_late(u) else peers)[s]}
        q_copies[s, u] = start(remote(q_send[s].at[u], q_recv[s].at[u], q_ss.at[s], q_rs.at[s, u], where))

    def read(s, u, k):
        p, h = units[u]
        if s > 0:
            return acc[s - 1][u, k]
        if is_late(u):
            return late_value(u, 2 * k + late_bits[0])
        return states[p, :, lanes(2 * k + bits[0], h)] * usable[p]

    def first_send(u):
        p, h = units[u]
        if is_late(u):
            send_values(0, u, [late_value(u, 2 * k + 1 - late_bits[0]) for k in range(half)], 1.0)
        else:
            values = [states[p, :, lanes(2 * k + 1 - bits[0], h)] for k in range(half)]
            send_values(0, u, values, usable[p])

    def fold(s, u):
        p, h = units[u]
        q_copies[s, u].wait_recv()
        bound = late_peer[s] if is_late(u) and s < 2 else bound_peer[s, p : p + 1]
        scale = tile_lanes(bound * (1.0 / FULL), piece)
        right = jnp.full((state_n, piece), bit_of(s, u), jnp.int32) == 1
        below = lax.rem(late_share(me) if is_late(u) else me, 1 << (s + 1))

        def folded(k):
            other = to_float(q_recv[s][u, k]) * scale
            own = read(s, u, k)
            if is_late(u) and s == 1:
                return own + other
            v = k * (1 << (s + 1)) + below
            share = late_share(v) if is_late(u) else v
            if is_late(u) and s == 0:
                late_at = (h - late_from) * piece
                behind = zd_sel[k][:, late_at : late_at + piece]
            else:
                behind = d_sel[s][k, p : p + 1, h * piece : (h + 1) * piece]
            decay = jnp.exp(-rates[:, lanes(share, h)] * behind)
            early = jnp.where(right, other, own)
            later = jnp.where(right, own, other)
            return decay * early + later

        if s + 1 < levels:
            bit = bit_of(s + 1, u)
            count = n >> (s + 2)
            send_values(s + 1, u, [folded(2 * k + 1 - bit) for k in range(count)], 1.0)
            for k in range(count):
                acc[s][u, k] = folded(2 * k + bit)
        else:
            at = pl.ds(h * piece, piece)
            handed[first + p, :, at] = folded(0)
            for k in range(1, nb):
                start(
                    remote(
                        handed.at[first + p, :, at],
                        handed.at[first + p, :, at],
                        hand_ss.at[k - 1],
                        hand_rs.at[k - 1],
                        {"batch": lax.rem(b + k, nb)},
                    )
                )

    if late_units:
        late_lanes = late_units * piece

        def late_row(v):
            at = late_share(v) * share_len + late_from * piece
            return steps[late_prompt, :, at : at + late_lanes]

        def late_rows():
            return jnp.concatenate([late_row(v) for v in range(n)], axis=0) * usable[late_prompt]

        zd_copies = [
            remote(zsteps_send, zsteps_recv, zd_ss.at[0], zd_rs.at[0], {"seq": peers[0]}),
            remote(zd_send, zd_recv, zd_ss.at[1], zd_rs.at[1], {"seq": late_peers[0]}),
        ]
        zsteps_send[...] = to_int16(late_rows() * STEP_UNIT)
        start(zd_copies[0])

        def late_value(u, v):
            h = units[u][1]
            at = lanes(late_share(v), h)
            late_at = (h - late_from) * piece
            decay = jnp.exp(-rates[:, at] * zpre[v][:, late_at : late_at + piece])
            return states[late_prompt, :, at] * (decay * usable[late_prompt])

        def late_begin():
            zd_copies[0].wait_recv()
            other = to_float(zsteps_recv[...]) * (1.0 / STEP_UNIT)
            before = jnp.where(jnp.full(other.shape, bits[0], jnp.int32) == 1, 0.0, other)
            for v in range(n):
                zpre[v] = before[v : v + 1]
            keep, send = split_rows(late_rows() + other, 1, late_bits[0])
            zd_keep[...] = keep
            zd_send[...] = to_int16(send * (STEP_UNIT / 2))
            start(zd_copies[1])

            late_own[0] = bound_own[0, late_prompt : late_prompt + 1]
            for u in late:
                first_send(u)

        def late_steps():
            zd_copies[1].wait_recv()
            own, other = zd_keep[...], to_float(zd_recv[...]) * (2 / STEP_UNIT)
            selected = jnp.where(jnp.full(own.shape, late_bits[0], jnp.int32) == 1, own, other)
            for k in range(half):
                zd_sel[k] = selected[k : k + 1]


    relays = [
        remote(
            arrived.at[b], arrived.at[b], relay_ss.at[k - 1], relay_rs.at[k - 1], {"batch": lax.rem(b + k, nb)}
        )
        for k in range(1, nb)
    ]

    top_width = min(512, share_len)
    for p in range(prompts):
        load_states[p].wait()

        def larger(i, top):
            at = pl.ds(pl.multiple_of(i * top_width, 128), top_width)
            return jnp.maximum(top, jnp.abs(states[p, :, at]))

        top = lax.fori_loop(0, channels // top_width, larger, jnp.zeros((state_n, top_width), jnp.float32), unroll=4)
        bound_own[0, p : p + 1] = jnp.maximum(lane_top([top]) * usable[p], 1e-30)
    table[me] = bound_own[0]
    for s in range(levels):
        for i in range(1 << s):
            to = bottom(peers[s], s) + i
            start(remote(bound_own.at[0], table.at[me], m_ss.at[0], m_rs.at[s], {"seq": to}))
    send_cache(1)
    for u in plain:
        first_send(u)

    shape3 = (positions, kv_heads, width)
    position = lax.broadcasted_iota(jnp.int32, shape3, 0) * n + me
    flat = positions * kv_heads
    column = lax.broadcasted_iota(jnp.int32, (heads, flat), 1)
    owner = lax.broadcasted_iota(jnp.int32, (heads, flat), 0) // group
    same_head = lax.rem(column, kv_heads) == owner
    column_position = (column // kv_heads) * n + me
    note_lane = lax.broadcasted_iota(jnp.int32, (heads, 128), 1)
    note_lane = note_lane - lax.rem(lax.broadcasted_iota(jnp.int32, (heads, 128), 0), own_heads)

    def attend(r):
        chosen, hits, length = pick(r, b, requests, all_prompts, plen, tslot, clen)
        fresh_limit = jnp.where(hits > 0, length, 0)
        new = arrived[chosen // prompts, :, lax.rem(chosen, prompts)].reshape(shape3).astype(jnp.float32)
        old = resident[r].astype(jnp.float32)
        x = jnp.where(position < fresh_limit, new, old)
        x = jnp.where(position < length, x, 0.0)
        x = jnp.where(position == length, token[r].astype(jnp.float32)[None], x)
        merged[r] = x.astype(jnp.bfloat16)
        x2 = x.reshape(flat, width)
        keys = x2[:, :head_dim].astype(jnp.bfloat16)
        values = x2[:, head_dim:].astype(jnp.bfloat16)
        score = lax.dot_general(
            queries[r], keys, (((1,), (1,)), ((), ())), preferred_element_type=jnp.float32
        ) * (1.0 / math.sqrt(head_dim))
        seen = same_head & (column_position <= length)
        score = jnp.where(seen, score, LOW)
        top = jnp.max(score, axis=1, keepdims=True)
        weight = jnp.where(seen, jnp.exp(score - top), 0.0)
        total = jnp.sum(weight, axis=1, keepdims=True)
        out = jnp.dot(weight.astype(jnp.bfloat16), values, preferred_element_type=jnp.float32)
        some = total > 0.0
        safe = jnp.where(some, total, 1.0)
        out = out / safe
        lse = jnp.where(some, top + jnp.log(safe), LOW)
        peak = jnp.maximum(jnp.max(jnp.abs(out), axis=1, keepdims=True), 1e-30)
        coded = jnp.round(out * (FULL / peak)).astype(jnp.int32)
        for j in range(n):
            osend[j, r * own_heads : (r + 1) * own_heads] = coded[j * own_heads : (j + 1) * own_heads].astype(jnp.int16)
        noted = jnp.where(note_lane == r * own_heads, lse, lse_all[...])
        lse_all[...] = jnp.where(note_lane == (requests + r) * own_heads, peak * (1.0 / FULL), noted)

    def attention_begin():
        settle(arrived.at[b, pl.ds(0, n - 1)], cache_rs.at[0])
        load_piece.wait()
        for copy in relays:
            start(copy)
        for copy in load_attention:
            copy.wait()
        lse_all[...] = jnp.zeros((heads, 128), jnp.float32)

    def send_out(ks):
        for k in ks:
            to = across(k)
            lse_send[to] = jnp.sum(lse_all[pl.ds(pl.multiple_of(to * own_heads, own_heads), own_heads)], axis=0, keepdims=True)
            start(remote(lse_send.at[to], lse_recv.at[me], l_ss.at[0], l_rs.at[0], {"seq": to}))
            start(remote(osend.at[to], orecv.at[me], o_ss.at[0], o_rs.at[0], {"seq": to}))

    def attention_end():
        send_out(range(n - 2, 0, -2))
        lse_recv[me] = jnp.sum(lse_all[pl.ds(pl.multiple_of(me * own_heads, own_heads), own_heads)], axis=0, keepdims=True)
        orecv[me] = osend[me]

    def attention_last():
        send_out(range(n - 1, 0, -2))

    load_rates.wait()

    def attend_some(r):
        if r == 0:
            for copy in relays:
                copy.wait_recv()
        attend(r)

    events = [(D_TIME + D_GAP * s, functools.partial(fold_steps, s)) for s in range(levels)]
    events += [(BOUND_TIME + BOUND_GAP * s, functools.partial(fold_bounds, s)) for s in range(levels)]
    events.append((RELAY_TIME, attention_begin))
    events.append((OUT_TIME, attention_end))
    events.append((OUT_TIME + OUT_GAP, attention_last))
    events += [(ATTEND_TIME + ATTEND_GAP * r, functools.partial(attend_some, r)) for r in range(requests)]
    for i, u in enumerate(plain):
        for s in range(levels):
            lag = FIRST_LAG + NEXT_LAG * (s - 1) if s else 0.0
            events.append((FOLD_TIME + FOLD_GAP * i + lag, functools.partial(fold, s, u)))
    if late_units:
        events.append((D_TIME + 0.1, late_begin))
        events.append((D_TIME + D_GAP + 0.1, late_steps))
        for i, u in enumerate(late):
            events.append((LATE_TIME + 0.1 * i, functools.partial(fold, 0, u)))
            for s in range(1, levels):
                expected = FOLD_TIME + FOLD_GAP * (len(plain) + i / 2) + LATE_GAP + LAST_GAP * (s - 1)
                events.append((expected, functools.partial(fold, s, u)))
    for _, event in sorted(events, key=lambda e: e[0]):
        event()

    for copy in load_through:
        copy.wait()
    others = pl.ds(0, n - 1)
    settle(lse_recv.at[others], l_rs.at[0])
    settle(orecv.at[others], o_rs.at[0])
    for k in range(1, nb):
        theirs = pl.ds(lax.rem(b + nb - k, nb) * prompts, prompts)
        settle(handed.at[theirs], hand_rs.at[k - 1])
        settle(handed.at[pl.ds(first, prompts)], hand_ss.at[k - 1])
    settle(arrived.at[b, others], cache_ss.at[0])
    settle(lse_send.at[others], l_ss.at[0])
    settle(osend.at[others], o_ss.at[0])
    for s in range(levels):
        settle(q_send[s], q_ss.at[s])
    settle(table.at[others], m_ss.at[0])
    for copy in relays + d_copies + (zd_copies if late_units else []):
        copy.wait_send()


def finish(dims, plen_hbm, tslot_hbm, clen_hbm, merged, handed, orecv, lse_recv, rates, rstates, dt, inner, gate, s_in, s_out, skip,
           merged_out, attention_out, nstates_out, mout_out, nstates, mout, attention, plen, tslot, clen, sems, scalar_sems):
    n, nb = dims
    b = lax.axis_index("batch")
    all_prompts = handed.shape[0]
    requests, state_n, share_len = rstates.shape
    own_heads, head_dim = attention.shape[1:]
    chunk = min(512, share_len)
    per_share = share_len // chunk

    scalar_copies = []
    for i, (src, dst) in enumerate(((plen_hbm, plen), (tslot_hbm, tslot), (clen_hbm, clen))):
        scalar_copies.append(pltpu.make_async_copy(src, dst, scalar_sems.at[i]))
        scalar_copies[-1].start()
    copies = []

    def out(src, dst, i):
        copy = pltpu.make_async_copy(src, dst, sems.at[i])
        copy.start()
        copies.append(copy)

    out(merged, merged_out, 0)
    eye = lax.broadcasted_iota(jnp.int32, (state_n, state_n), 0) == lax.broadcasted_iota(
        jnp.int32, (state_n, state_n), 1
    )

    def as_column(row):
        spread = jnp.where(eye, jnp.broadcast_to(row, (state_n, state_n)), 0.0)
        return jnp.sum(spread, axis=1, keepdims=True)

    note_lane = lax.broadcasted_iota(jnp.int32, (n, own_heads, 128), 2)
    note_lane = note_lane - lax.broadcasted_iota(jnp.int32, (n, own_heads, 128), 1)
    noted = jnp.broadcast_to(lse_recv[...], (n, own_heads, 128))
    for r in range(requests):
        lse = jnp.sum(jnp.where(note_lane == r * own_heads, noted, 0.0), axis=2, keepdims=True)
        unit = jnp.sum(jnp.where(note_lane == (requests + r) * own_heads, noted, 0.0), axis=2, keepdims=True)
        share = jnp.exp(lse - jnp.max(lse, axis=0, keepdims=True))
        parts = to_float(orecv[:, r * own_heads : (r + 1) * own_heads])
        top = jnp.sum(share * unit * parts, axis=0)
        attention[r] = (top / jnp.sum(share, axis=0)).astype(jnp.bfloat16)
    out(attention, attention_out, 2)
    for copy in scalar_copies:
        copy.wait()
    picks = [pick(r, b, requests, all_prompts, plen, tslot, clen) for r in range(requests)]
    in_all, out_all = s_in[...], s_out[...]
    in_cols = [as_column(in_all[r : r + 1]) for r in range(requests)]
    out_cols = [as_column(out_all[r : r + 1]) for r in range(requests)]

    for c in range(per_share):
        at = pl.ds(c * chunk, chunk)
        step_rows = dt[:, at]
        x_rows = inner[:, at].astype(jnp.float32)
        g = gate[:, at].astype(jnp.float32)
        rate = -rates[:, at]
        push_rows = step_rows * x_rows
        out_rows = []
        for r in range(requests):
            chosen, hits, _ = picks[r]
            fresh = jnp.full((state_n, chunk), hits, jnp.int32) > 0
            begin = jnp.where(fresh, handed[chosen, :, at], rstates[r, :, at])
            after = jnp.exp(rate * step_rows[r : r + 1]) * begin
            after = after + push_rows[r : r + 1] * in_cols[r]
            nstates[r, :, at] = after
            out_rows.append(jnp.sum(out_cols[r] * after, axis=0, keepdims=True))
        out(nstates.at[:, :, at], nstates_out.at[:, :, at], 3 + c)
        read_out = jnp.concatenate(out_rows, axis=0) + skip[:, at] * x_rows
        mout[:, at] = (read_out * (g / (1.0 + jnp.exp(-g)))).astype(jnp.bfloat16)
    out(mout, mout_out, 1)

    for copy in copies:
        copy.wait()


def local(
    n,
    nb,
    prompt_cache,
    prompt_states,
    block_steps,
    prompt_lengths,
    target_slots,
    cache_lengths,
    resident_cache,
    token_cache,
    queries,
    resident_states,
    decay_rates,
    step_sizes,
    inner_input,
    inner_gate,
    state_input,
    state_readout,
    skip_gain,
):
    levels = n.bit_length() - 1
    prompts, block_len, kv_heads, width = prompt_cache.shape
    requests, heads, head_dim = queries.shape
    state_n, channels = decay_rates.shape
    share = channels // n
    piece = share // PIECES
    own_heads = heads // n
    positions = resident_cache.shape[1]
    all_prompts = prompts * nb
    rows = block_len // n
    unit_count = prompts * PIECES
    late_units = LATE
    f32, bf16, i16 = jnp.float32, jnp.bfloat16, jnp.int16
    vmem = pl.BlockSpec(memory_space=pltpu.VMEM)
    hbm = pl.BlockSpec(memory_space=pltpu.HBM)
    dma = pltpu.SemaphoreType.DMA
    halves = [n >> (s + 1) for s in range(levels)]
    through = (resident_states, step_sizes, inner_input, inner_gate, state_input, state_readout, skip_gain[None])
    operands = (
        prompt_cache.reshape(prompts, rows, n, kv_heads, width),
        prompt_states[:, 0],
        block_steps,
        resident_cache[:, :, 0],
        token_cache,
        queries,
        decay_rates,
    ) + through
    outs = (
        pltpu.VMEM((requests, positions, kv_heads, width), bf16),
        pltpu.VMEM((all_prompts, state_n, share), f32),
        pltpu.VMEM((n, requests * own_heads, head_dim), i16),
        pltpu.VMEM((n, 1, 128), f32),
        pltpu.VMEM((state_n, share), f32),
    ) + tuple(pltpu.VMEM(x.shape, x.dtype) for x in through)
    scratch = [
        pltpu.VMEM((nb, n, prompts, rows, kv_heads, width), bf16),
        pltpu.VMEM((prompts, state_n, channels), f32),
        pltpu.VMEM(block_steps.shape, f32),
        pltpu.VMEM((requests, positions, kv_heads, width), bf16),
        pltpu.VMEM(token_cache.shape, bf16),
        pltpu.VMEM(queries.shape, bf16),
        pltpu.VMEM(decay_rates.shape, f32),
        pltpu.VMEM((n, requests * own_heads, head_dim), i16),
        pltpu.VMEM((heads, 128), f32),
        pltpu.VMEM((n, 1, 128), f32),
        pltpu.SMEM(prompt_lengths.shape, jnp.int32),
        pltpu.SMEM(target_slots.shape, jnp.int32),
        pltpu.SMEM(cache_lengths.shape, jnp.int32),
        dma((10,)),
        dma((prompts,)),
        dma((len(through),)),
    ]
    for _ in range(2):
        scratch += [pltpu.VMEM((h * prompts, share), i16) for h in halves]
    scratch += [pltpu.VMEM((h, prompts, share), f32) for h in halves]
    scratch += [pltpu.VMEM((h * prompts, share), f32) for h in halves[1:]]
    for _ in range(2):
        scratch += [pltpu.VMEM((unit_count, h, state_n, piece), i16) for h in halves]
    scratch += [pltpu.VMEM((unit_count, h, state_n, piece), f32) for h in halves[1:]]
    scratch += [pltpu.VMEM((n, prompts, 128), f32)]
    scratch += [pltpu.VMEM((levels, prompts, 128), f32)] * 2
    if late_units:
        late_lanes = late_units * piece
        scratch += [pltpu.VMEM((2, 1, 128), f32)] * 2
        scratch += [pltpu.VMEM((n, late_lanes), i16)] * 2
        scratch += [pltpu.VMEM((n, 1, late_lanes), f32)]
        scratch += [pltpu.VMEM((n // 2, late_lanes), i16)] * 2
        scratch += [pltpu.VMEM((n // 2, 1, late_lanes), f32)]
        scratch += [pltpu.VMEM((n // 2, late_lanes), f32)]
        scratch += [dma((2,))] * 2
    scratch += [dma((1,))] * 2
    scratch += [dma((max(nb - 1, 1),))] * 2
    scratch += [dma((levels,))] * 2
    scratch += [dma((levels,)), dma((levels, unit_count))]
    scratch += [dma((1,)), dma((levels,))]
    scratch += [dma((max(nb - 1, 1),))] * 2
    scratch += [dma((1,))] * 4
    scalars = [
        pltpu.with_memory_space_constraint(x, pltpu.HBM)
        for x in (prompt_lengths, target_slots, cache_lengths)
    ]
    parts = pl.pallas_call(
        functools.partial(exchange, (n, nb, levels, block_len, late_units)),
        out_shape=outs,
        in_specs=[hbm] * (3 + len(operands)),
        out_specs=(vmem,) * len(outs),
        scratch_shapes=scratch,
        compiler_params=pltpu.CompilerParams(
            collective_id=0, has_side_effects=True, vmem_limit_bytes=40 << 20
        ),
    )(*scalars, *(pltpu.with_memory_space_constraint(x, pltpu.HBM) for x in operands))
    chunks = share // min(512, share)
    merged, attention, next_states, mamba_output = pl.pallas_call(
        functools.partial(finish, (n, nb)),
        out_shape=(
            jax.ShapeDtypeStruct((requests, positions, kv_heads, width), bf16),
            jax.ShapeDtypeStruct((requests, own_heads, head_dim), bf16),
            jax.ShapeDtypeStruct((requests, state_n, share), f32),
            jax.ShapeDtypeStruct((requests, share), bf16),
        ),
        in_specs=[hbm] * 3 + [vmem] * len(parts),
        out_specs=(hbm,) * 4,
        scratch_shapes=[
            pltpu.VMEM((requests, state_n, share), f32),
            pltpu.VMEM((requests, share), bf16),
            pltpu.VMEM((requests, own_heads, head_dim), bf16),
            *(pltpu.SMEM(x.shape, jnp.int32) for x in scalars),
            dma((3 + chunks,)),
            dma((3,)),
        ],
        compiler_params=pltpu.CompilerParams(vmem_limit_bytes=16 << 20),
    )(*scalars, *parts)
    return merged[:, :, None], attention, next_states, mamba_output


def solution(mesh):
    n, nb = mesh.shape["seq"], mesh.shape["batch"]
    return jax.shard_map(
        functools.partial(local, n, nb),
        mesh=mesh,
        in_specs=(
            P(("groups", "batch"), "seq", None, None),
            P(("groups", "batch"), "seq", None, None),
            P(("groups", "batch"), "seq", None),
            P("groups"),
            P("groups"),
            P(("groups", "batch")),
            P(("groups", "batch"), None, "seq", None, None),
            P(("groups", "batch"), None, None),
            P(("groups", "batch"), None, None),
            P(("groups", "batch"), None, "seq"),
            P(),
            P(("groups", "batch"), "seq"),
            P(("groups", "batch"), "seq"),
            P(("groups", "batch"), "seq"),
            P(("groups", "batch"), None),
            P(("groups", "batch"), None),
            P("seq"),
        ),
        out_specs=(
            P(("groups", "batch"), None, "seq", None, None),
            P(("groups", "batch"), "seq", None),
            P(("groups", "batch"), None, "seq"),
            P(("groups", "batch"), "seq"),
        ),
        check_vma=False,
    )
```

```python
import functools
import math

import jax
import jax.numpy as jnp
from jax import lax
from jax.experimental import pallas as pl
from jax.experimental.pallas import tpu as pltpu
from jax.sharding import PartitionSpec as P

MESH = pl.DeviceIdType.MESH
FULL = 32760.0
LOW = -1e30
PIECES = 4
LATE = 2
STEP_UNIT = float(1 << 18)
D_TIME, D_GAP = 4.5, 4.6
BOUND_TIME, BOUND_GAP = 6.5, 3.5
RELAY_TIME, ATTEND_TIME, ATTEND_GAP = 14.5, 15.5, 0.5
OUT_TIME, OUT_GAP = 19.5, 0.05
FOLD_TIME, FOLD_GAP, FIRST_LAG, NEXT_LAG = 8.8, 1.39, 5.5, 5.5
LATE_TIME, LATE_GAP, LAST_GAP = 13.0, 0.5, 4.0


def to_int16(value):
    return jnp.round(value).astype(jnp.int32).astype(jnp.int16)


def to_float(value):
    return value.astype(jnp.int32).astype(jnp.float32)


def tile_lanes(row, width):
    return jnp.concatenate([row] * (width // 128), axis=1)


def lane_top(values):
    top = jnp.abs(values[0])
    for value in values[1:]:
        top = jnp.maximum(top, jnp.abs(value))
    parts = [top[:, i : i + 128] for i in range(0, top.shape[1], 128)]
    top = parts[0]
    for part in parts[1:]:
        top = jnp.maximum(top, part)
    return jnp.maximum(jnp.max(top, axis=0, keepdims=True), 1e-30)


def split_rows(value, size, bit):
    count = value.shape[0] // size
    even = [value[k * size : (k + 1) * size] for k in range(0, count, 2)]
    odd = [value[k * size : (k + 1) * size] for k in range(1, count, 2)]
    even = jnp.concatenate(even, axis=0) if len(even) > 1 else even[0]
    odd = jnp.concatenate(odd, axis=0) if len(odd) > 1 else odd[0]
    right = jnp.full(even.shape, bit, jnp.int32) == 1
    return jnp.where(right, odd, even), jnp.where(right, even, odd)


def pick(r, b, requests, all_prompts, plen, tslot, clen):
    slot = b * requests + r
    chosen, length, hits = jnp.int32(0), jnp.int32(0), jnp.int32(0)
    for p in range(all_prompts):
        hit = tslot[p] == slot
        chosen = jnp.where(hit, p, chosen)
        length = jnp.where(hit, plen[p], length)
        hits = jnp.where(hit, 1, hits)
    return chosen, hits, jnp.where(hits > 0, length, clen[r])


def exchange(dims, *refs):
    n, nb, levels, block_len, late_units = dims
    refs = list(refs)

    def take(count):
        out = refs[:count]
        del refs[:count]
        return out

    scalar_hbm = take(3)
    cache_hbm, states_hbm, steps_hbm, resident_hbm, token_hbm, queries_hbm, rates_hbm = take(7)
    through_hbm = take(7)
    merged, handed, attention, rates_own = take(4)
    through = take(7)
    arrived, states, steps, resident, token, queries, rates, osend, lse_all, lse_send = take(10)
    orecv, lse_recv = take(2)
    plen, tslot, clen = scalars = take(3)
    load_sems, state_sems, through_sems = take(3)
    d_send, d_recv, d_sel = take(levels), take(levels), take(levels)
    d_keep = take(levels - 1)
    q_send, q_recv = take(levels), take(levels)
    acc = take(levels - 1)
    table, bound_own, bound_peer = take(3)
    if late_units:
        late_own, late_peer, zsteps_send, zsteps_recv, zpre = take(5)
        zd_send, zd_recv, zd_sel, zd_keep = take(4)
        zd_ss, zd_rs = take(2)
    (
        cache_ss, cache_rs, relay_ss, relay_rs, d_ss, d_rs, q_ss, q_rs, m_ss, m_rs,
        hand_ss, hand_rs, o_ss, o_rs, l_ss, l_rs,
    ) = refs

    me = lax.axis_index("seq")
    b = lax.axis_index("batch")
    prompts, rows, _, kv_heads, width = cache_hbm.shape
    all_prompts = prompts * nb
    requests, heads, head_dim = queries.shape
    state_n, channels = rates.shape
    share_len = channels // n
    piece = share_len // PIECES
    own_heads = heads // n
    group = heads // kv_heads
    positions = resident.shape[1]
    bits = [lax.rem(me // (1 << s), 2) for s in range(levels)]
    peers = [me + (1 - 2 * bits[s]) * (1 << s) for s in range(levels)]
    first = b * prompts

    barrier = pltpu.get_barrier_semaphore()
    for k in range(1, n):
        pl.semaphore_signal(barrier, inc=1, device_id={"seq": lax.rem(me + k, n)}, device_id_type=MESH)
    for k in range(1, nb):
        pl.semaphore_signal(barrier, inc=1, device_id={"batch": lax.rem(b + k, nb)}, device_id_type=MESH)

    def load(src, dst, sem):
        copy = pltpu.make_async_copy(src, dst, sem)
        copy.start()
        return copy

    load_scalars = [load(src, dst, load_sems.at[6 + i]) for i, (src, dst) in enumerate(zip(scalar_hbm, scalars))]
    load_steps = load(steps_hbm, steps, load_sems.at[0])
    load_states = [load(states_hbm.at[0], states.at[0], state_sems.at[0])]
    load_piece = load(cache_hbm.at[:, :, me], arrived.at[b, me], load_sems.at[9])
    load_rates = load(rates_hbm, rates, load_sems.at[1])
    for p in range(1, prompts):
        load_states.append(load(states_hbm.at[p], states.at[p], state_sems.at[p]))
    load_attention = [
        load(resident_hbm, resident, load_sems.at[2]),
        load(token_hbm, token, load_sems.at[3]),
        load(queries_hbm, queries, load_sems.at[4]),
    ]
    own_lanes = pl.ds(pl.multiple_of(me * share_len, 128), share_len)
    load_through = [load(rates_hbm.at[:, own_lanes], rates_own, load_sems.at[5])]
    for i, (src, dst) in enumerate(zip(through_hbm, through)):
        load_through.append(load(src, dst, through_sems.at[i]))

    def remote(src, dst, ss, rs, where):
        return pltpu.make_async_remote_copy(
            src_ref=src, dst_ref=dst, send_sem=ss, recv_sem=rs, device_id=where, device_id_type=MESH
        )

    def start(copy):
        copy.start()
        return copy

    def settle(ref, sem):
        pltpu.make_async_copy(ref, ref, sem).wait()

    def lanes(share, h):
        return pl.ds(pl.multiple_of(share * share_len + h * piece, 128), piece)

    pl.semaphore_wait(barrier, n - 1 + nb - 1)

    def across(k):
        to = me
        for i in range(levels):
            if (k >> i) % 2:
                to = to + peers[i] - me
        return to

    def send_cache(k):
        to = across(k)
        start(remote(cache_hbm.at[:, :, to], arrived.at[b, me], cache_ss.at[0], cache_rs.at[0], {"seq": to}))

    for k in range(n - 1, 1, -2):
        send_cache(k)
    for k in range(n - 2, 0, -2):
        send_cache(k)

    for copy in load_scalars:
        copy.wait()
    usable = [
        jnp.where(me * block_len < plen[first + p], 1.0, 0.0).astype(jnp.float32)
        for p in range(prompts)
    ]

    step_width = min(512, share_len)
    row_id = lax.broadcasted_iota(jnp.int32, (prompts, step_width), 0)
    usable_rows = jnp.zeros((prompts, step_width), jnp.float32)
    for p in range(prompts):
        usable_rows = jnp.where(row_id == p, usable[p], usable_rows)

    def step_rows(bit, c):
        parts = []
        for k in range(n // 2):
            at = pl.ds(pl.multiple_of((2 * k + bit) * share_len + c * step_width, 128), step_width)
            parts.append(jnp.concatenate([steps[p, :, at] for p in range(prompts)], axis=0) * usable_rows)
        return jnp.concatenate(parts, axis=0)

    def columns(c):
        return pl.ds(pl.multiple_of(c * step_width, 128), step_width)

    d_copies = [
        remote(d_send[s], d_recv[s], d_ss.at[s], d_rs.at[s], {"seq": peers[s]}) for s in range(levels)
    ]
    load_steps.wait()

    @pl.loop(0, share_len // step_width)
    def _(c):
        d_send[0][:, columns(c)] = to_int16(step_rows(1 - bits[0], c) * STEP_UNIT)

    start(d_copies[0])

    def fold_steps(s):
        d_copies[s].wait_recv()

        @pl.loop(0, share_len // step_width)
        def _(c):
            at = columns(c)
            other = to_float(d_recv[s][:, at]) * ((1 << s) / STEP_UNIT)
            own = step_rows(bits[0], c) if s == 0 else d_keep[s - 1][:, at]
            selected = jnp.where(jnp.full(own.shape, bits[s], jnp.int32) == 1, own, other)
            for k in range(n >> (s + 1)):
                d_sel[s][k, :, at] = selected[k * prompts : (k + 1) * prompts]
            if s + 1 < levels:
                keep, send = split_rows(own + other, prompts, bits[s + 1])
                d_keep[s][:, at] = keep
                d_send[s + 1][:, at] = to_int16(send * (STEP_UNIT / (1 << (s + 1))))

        if s + 1 < levels:
            start(d_copies[s + 1])

    def bottom(device, s):
        return device - lax.rem(device, 1 << s)

    def fold_bounds(s):
        settle(table.at[pl.ds(0, 1 << s)], m_rs.at[s])

        def group_bound(device):
            total = table[bottom(device, s)]
            for i in range(1, 1 << s):
                total = total + table[bottom(device, s) + i]
            return total

        bound_peer[s] = group_bound(peers[s])
        if s + 1 < levels:
            bound_own[s + 1] = bound_own[s] + bound_peer[s]
        if late_units and s == 1:
            at = slice(late_prompt, late_prompt + 1)
            late_own[1] = table[me, at] + table[peers[1], at]
            late_peer[0] = table[peers[1], at]
            late_peer[1] = table[peers[0], at] + table[peers[0] + peers[1] - me, at]

    half = n // 2
    late_bits = [bits[1], bits[0]] + bits[2:]
    late_peers = [peers[1], peers[0]] + peers[2:]
    units = [(p, h) for p in range(prompts) for h in range(PIECES)]
    total_units = len(units)
    plain = list(range(total_units - late_units))
    late = list(range(total_units - late_units, total_units))
    late_prompt = prompts - 1
    late_from = PIECES - late_units

    def is_late(u):
        return u >= total_units - late_units

    def bit_of(s, u):
        return late_bits[s] if is_late(u) else bits[s]

    def late_share(v):
        return (v // 4) * 4 + (v % 2) * 2 + (v // 2) % 2

    q_copies = {}

    def send_values(s, u, values, factor):
        bound = late_own[s] if is_late(u) and s < 2 else bound_own[s, units[u][0] : units[u][0] + 1]
        scale = tile_lanes(FULL / bound * factor, piece)
        for k, value in enumerate(values):
            q_send[s][u, k] = to_int16(value * scale)
        where = {"seq": (late_peers if is_late(u) else peers)[s]}
        q_copies[s, u] = start(remote(q_send[s].at[u], q_recv[s].at[u], q_ss.at[s], q_rs.at[s, u], where))

    def read(s, u, k):
        p, h = units[u]
        if s > 0:
            return acc[s - 1][u, k]
        if is_late(u):
            return late_value(u, 2 * k + late_bits[0])
        return states[p, :, lanes(2 * k + bits[0], h)] * usable[p]

    def first_send(u):
        p, h = units[u]
        if is_late(u):
            send_values(0, u, [late_value(u, 2 * k + 1 - late_bits[0]) for k in range(half)], 1.0)
        else:
            values = [states[p, :, lanes(2 * k + 1 - bits[0], h)] for k in range(half)]
            send_values(0, u, values, usable[p])

    def fold(s, u):
        p, h = units[u]
        q_copies[s, u].wait_recv()
        bound = late_peer[s] if is_late(u) and s < 2 else bound_peer[s, p : p + 1]
        scale = tile_lanes(bound * (1.0 / FULL), piece)
        right = jnp.full((state_n, piece), bit_of(s, u), jnp.int32) == 1
        below = lax.rem(late_share(me) if is_late(u) else me, 1 << (s + 1))

        def folded(k):
            other = to_float(q_recv[s][u, k]) * scale
            own = read(s, u, k)
            if is_late(u) and s == 1:
                return own + other
            v = k * (1 << (s + 1)) + below
            share = late_share(v) if is_late(u) else v
            if is_late(u) and s == 0:
                late_at = (h - late_from) * piece
                behind = zd_sel[k][:, late_at : late_at + piece]
            else:
                behind = d_sel[s][k, p : p + 1, h * piece : (h + 1) * piece]
            decay = jnp.exp(-rates[:, lanes(share, h)] * behind)
            early = jnp.where(right, other, own)
            later = jnp.where(right, own, other)
            return decay * early + later

        if s + 1 < levels:
            bit = bit_of(s + 1, u)
            count = n >> (s + 2)
            send_values(s + 1, u, [folded(2 * k + 1 - bit) for k in range(count)], 1.0)
            for k in range(count):
                acc[s][u, k] = folded(2 * k + bit)
        else:
            at = pl.ds(h * piece, piece)
            handed[first + p, :, at] = folded(0)
            for k in range(1, nb):
                start(
                    remote(
                        handed.at[first + p, :, at],
                        handed.at[first + p, :, at],
                        hand_ss.at[k - 1],
                        hand_rs.at[k - 1],
                        {"batch": lax.rem(b + k, nb)},
                    )
                )

    if late_units:
        late_lanes = late_units * piece

        def late_row(v):
            at = late_share(v) * share_len + late_from * piece
            return steps[late_prompt, :, at : at + late_lanes]

        def late_rows():
            return jnp.concatenate([late_row(v) for v in range(n)], axis=0) * usable[late_prompt]

        zd_copies = [
            remote(zsteps_send, zsteps_recv, zd_ss.at[0], zd_rs.at[0], {"seq": peers[0]}),
            remote(zd_send, zd_recv, zd_ss.at[1], zd_rs.at[1], {"seq": late_peers[0]}),
        ]
        zsteps_send[...] = to_int16(late_rows() * STEP_UNIT)
        start(zd_copies[0])

        def late_value(u, v):
            h = units[u][1]
            at = lanes(late_share(v), h)
            late_at = (h - late_from) * piece
            decay = jnp.exp(-rates[:, at] * zpre[v][:, late_at : late_at + piece])
            return states[late_prompt, :, at] * (decay * usable[late_prompt])

        def late_begin():
            zd_copies[0].wait_recv()
            other = to_float(zsteps_recv[...]) * (1.0 / STEP_UNIT)
            before = jnp.where(jnp.full(other.shape, bits[0], jnp.int32) == 1, 0.0, other)
            for v in range(n):
                zpre[v] = before[v : v + 1]
            keep, send = split_rows(late_rows() + other, 1, late_bits[0])
            zd_keep[...] = keep
            zd_send[...] = to_int16(send * (STEP_UNIT / 2))
            start(zd_copies[1])

            late_own[0] = bound_own[0, late_prompt : late_prompt + 1]
            for u in late:
                first_send(u)

        def late_steps():
            zd_copies[1].wait_recv()
            own, other = zd_keep[...], to_float(zd_recv[...]) * (2 / STEP_UNIT)
            selected = jnp.where(jnp.full(own.shape, late_bits[0], jnp.int32) == 1, own, other)
            for k in range(half):
                zd_sel[k] = selected[k : k + 1]


    relays = [
        remote(
            arrived.at[b], arrived.at[b], relay_ss.at[k - 1], relay_rs.at[k - 1], {"batch": lax.rem(b + k, nb)}
        )
        for k in range(1, nb)
    ]

    top_width = min(512, share_len)
    for p in range(prompts):
        load_states[p].wait()

        def larger(i, top):
            at = pl.ds(pl.multiple_of(i * top_width, 128), top_width)
            return jnp.maximum(top, jnp.abs(states[p, :, at]))

        top = lax.fori_loop(0, channels // top_width, larger, jnp.zeros((state_n, top_width), jnp.float32), unroll=4)
        bound_own[0, p : p + 1] = jnp.maximum(lane_top([top]) * usable[p], 1e-30)
    table[me] = bound_own[0]
    for s in range(levels):
        for i in range(1 << s):
            to = bottom(peers[s], s) + i
            start(remote(bound_own.at[0], table.at[me], m_ss.at[0], m_rs.at[s], {"seq": to}))
    send_cache(1)
    for u in plain:
        first_send(u)

    shape3 = (positions, kv_heads, width)
    position = lax.broadcasted_iota(jnp.int32, shape3, 0) * n + me
    flat = positions * kv_heads
    column = lax.broadcasted_iota(jnp.int32, (heads, flat), 1)
    owner = lax.broadcasted_iota(jnp.int32, (heads, flat), 0) // group
    same_head = lax.rem(column, kv_heads) == owner
    column_position = (column // kv_heads) * n + me
    note_lane = lax.broadcasted_iota(jnp.int32, (heads, 128), 1)
    note_lane = note_lane - lax.rem(lax.broadcasted_iota(jnp.int32, (heads, 128), 0), own_heads)

    def attend(r):
        chosen, hits, length = pick(r, b, requests, all_prompts, plen, tslot, clen)
        fresh_limit = jnp.where(hits > 0, length, 0)
        new = arrived[chosen // prompts, :, lax.rem(chosen, prompts)].reshape(shape3).astype(jnp.float32)
        old = resident[r].astype(jnp.float32)
        x = jnp.where(position < fresh_limit, new, old)
        x = jnp.where(position < length, x, 0.0)
        x = jnp.where(position == length, token[r].astype(jnp.float32)[None], x)
        merged[r] = x.astype(jnp.bfloat16)
        x2 = x.reshape(flat, width)
        keys = x2[:, :head_dim].astype(jnp.bfloat16)
        values = x2[:, head_dim:].astype(jnp.bfloat16)
        score = lax.dot_general(
            queries[r], keys, (((1,), (1,)), ((), ())), preferred_element_type=jnp.float32
        ) * (1.0 / math.sqrt(head_dim))
        seen = same_head & (column_position <= length)
        score = jnp.where(seen, score, LOW)
        top = jnp.max(score, axis=1, keepdims=True)
        weight = jnp.where(seen, jnp.exp(score - top), 0.0)
        total = jnp.sum(weight, axis=1, keepdims=True)
        out = jnp.dot(weight.astype(jnp.bfloat16), values, preferred_element_type=jnp.float32)
        some = total > 0.0
        safe = jnp.where(some, total, 1.0)
        out = out / safe
        lse = jnp.where(some, top + jnp.log(safe), LOW)
        peak = jnp.maximum(jnp.max(jnp.abs(out), axis=1, keepdims=True), 1e-30)
        coded = jnp.round(out * (FULL / peak)).astype(jnp.int32)
        for j in range(n):
            osend[j, r * own_heads : (r + 1) * own_heads] = coded[j * own_heads : (j + 1) * own_heads].astype(jnp.int16)
        noted = jnp.where(note_lane == r * own_heads, lse, lse_all[...])
        lse_all[...] = jnp.where(note_lane == (requests + r) * own_heads, peak * (1.0 / FULL), noted)

    def attention_begin():
        settle(arrived.at[b, pl.ds(0, n - 1)], cache_rs.at[0])
        load_piece.wait()
        for copy in relays:
            start(copy)
        for copy in load_attention:
            copy.wait()
        lse_all[...] = jnp.zeros((heads, 128), jnp.float32)

    def send_out(ks):
        for k in ks:
            to = across(k)
            lse_send[to] = jnp.sum(lse_all[pl.ds(pl.multiple_of(to * own_heads, own_heads), own_heads)], axis=0, keepdims=True)
            start(remote(lse_send.at[to], lse_recv.at[me], l_ss.at[0], l_rs.at[0], {"seq": to}))
            start(remote(osend.at[to], orecv.at[me], o_ss.at[0], o_rs.at[0], {"seq": to}))

    def attention_end():
        send_out(range(n - 2, 0, -2))
        lse_recv[me] = jnp.sum(lse_all[pl.ds(pl.multiple_of(me * own_heads, own_heads), own_heads)], axis=0, keepdims=True)
        orecv[me] = osend[me]

    def attention_last():
        send_out(range(n - 1, 0, -2))

    load_rates.wait()

    def attend_some(r):
        if r == 0:
            for copy in relays:
                copy.wait_recv()
        attend(r)

    events = [(D_TIME + D_GAP * s, functools.partial(fold_steps, s)) for s in range(levels)]
    events += [(BOUND_TIME + BOUND_GAP * s, functools.partial(fold_bounds, s)) for s in range(levels)]
    events.append((RELAY_TIME, attention_begin))
    events.append((OUT_TIME, attention_end))
    events.append((OUT_TIME + OUT_GAP, attention_last))
    events += [(ATTEND_TIME + ATTEND_GAP * r, functools.partial(attend_some, r)) for r in range(requests)]
    for i, u in enumerate(plain):
        for s in range(levels):
            lag = FIRST_LAG + NEXT_LAG * (s - 1) if s else 0.0
            events.append((FOLD_TIME + FOLD_GAP * i + lag, functools.partial(fold, s, u)))
    if late_units:
        events.append((D_TIME + 0.1, late_begin))
        events.append((D_TIME + D_GAP + 0.1, late_steps))
        for i, u in enumerate(late):
            events.append((LATE_TIME + 0.1 * i, functools.partial(fold, 0, u)))
            for s in range(1, levels):
                expected = FOLD_TIME + FOLD_GAP * (len(plain) + i / 2) + LATE_GAP + LAST_GAP * (s - 1)
                events.append((expected, functools.partial(fold, s, u)))
    for _, event in sorted(events, key=lambda e: e[0]):
        event()

    for copy in load_through:
        copy.wait()
    others = pl.ds(0, n - 1)
    settle(lse_recv.at[others], l_rs.at[0])
    settle(orecv.at[others], o_rs.at[0])
    head_lane = lax.broadcasted_iota(jnp.int32, (n, own_heads, 128), 2)
    head_lane = head_lane - lax.broadcasted_iota(jnp.int32, (n, own_heads, 128), 1)
    noted = jnp.broadcast_to(lse_recv[...], (n, own_heads, 128))
    for r in range(requests):
        lse = jnp.sum(jnp.where(head_lane == r * own_heads, noted, 0.0), axis=2, keepdims=True)
        unit = jnp.sum(jnp.where(head_lane == (requests + r) * own_heads, noted, 0.0), axis=2, keepdims=True)
        share = jnp.exp(lse - jnp.max(lse, axis=0, keepdims=True))
        parts = to_float(orecv[:, r * own_heads : (r + 1) * own_heads])
        top = jnp.sum(share * unit * parts, axis=0)
        attention[r] = (top / jnp.sum(share, axis=0)).astype(jnp.bfloat16)
    for k in range(1, nb):
        theirs = pl.ds(lax.rem(b + nb - k, nb) * prompts, prompts)
        settle(handed.at[theirs], hand_rs.at[k - 1])
        settle(handed.at[pl.ds(first, prompts)], hand_ss.at[k - 1])
    settle(arrived.at[b, others], cache_ss.at[0])
    settle(lse_send.at[others], l_ss.at[0])
    settle(osend.at[others], o_ss.at[0])
    for s in range(levels):
        settle(q_send[s], q_ss.at[s])
    settle(table.at[others], m_ss.at[0])
    for copy in relays + d_copies + (zd_copies if late_units else []):
        copy.wait_send()


def finish(dims, plen_hbm, tslot_hbm, clen_hbm, merged, handed, attention, rates, rstates, dt, inner, gate, s_in, s_out, skip,
           merged_out, attention_out, nstates_out, mout_out, nstates, mout, plen, tslot, clen, sems, scalar_sems):
    n, nb = dims
    b = lax.axis_index("batch")
    all_prompts = handed.shape[0]
    requests, state_n, share_len = rstates.shape
    chunk = min(512, share_len)
    per_share = share_len // chunk

    scalar_copies = []
    for i, (src, dst) in enumerate(((plen_hbm, plen), (tslot_hbm, tslot), (clen_hbm, clen))):
        scalar_copies.append(pltpu.make_async_copy(src, dst, scalar_sems.at[i]))
        scalar_copies[-1].start()
    copies = []

    def out(src, dst, i):
        copy = pltpu.make_async_copy(src, dst, sems.at[i])
        copy.start()
        copies.append(copy)

    out(merged, merged_out, 0)
    out(attention, attention_out, 2)
    eye = lax.broadcasted_iota(jnp.int32, (state_n, state_n), 0) == lax.broadcasted_iota(
        jnp.int32, (state_n, state_n), 1
    )

    def as_column(row):
        spread = jnp.where(eye, jnp.broadcast_to(row, (state_n, state_n)), 0.0)
        return jnp.sum(spread, axis=1, keepdims=True)

    in_all, out_all = s_in[...], s_out[...]
    in_cols = [as_column(in_all[r : r + 1]) for r in range(requests)]
    out_cols = [as_column(out_all[r : r + 1]) for r in range(requests)]
    for copy in scalar_copies:
        copy.wait()
    picks = [pick(r, b, requests, all_prompts, plen, tslot, clen) for r in range(requests)]

    for c in range(per_share):
        at = pl.ds(c * chunk, chunk)
        step_rows = dt[:, at]
        x_rows = inner[:, at].astype(jnp.float32)
        g = gate[:, at].astype(jnp.float32)
        rate = -rates[:, at]
        push_rows = step_rows * x_rows
        out_rows = []
        for r in range(requests):
            chosen, hits, _ = picks[r]
            fresh = jnp.full((state_n, chunk), hits, jnp.int32) > 0
            begin = jnp.where(fresh, handed[chosen, :, at], rstates[r, :, at])
            after = jnp.exp(rate * step_rows[r : r + 1]) * begin
            after = after + push_rows[r : r + 1] * in_cols[r]
            nstates[r, :, at] = after
            out_rows.append(jnp.sum(out_cols[r] * after, axis=0, keepdims=True))
        out(nstates.at[:, :, at], nstates_out.at[:, :, at], 3 + c)
        read_out = jnp.concatenate(out_rows, axis=0) + skip[:, at] * x_rows
        mout[:, at] = (read_out * (g / (1.0 + jnp.exp(-g)))).astype(jnp.bfloat16)
    out(mout, mout_out, 1)

    for copy in copies:
        copy.wait()


def local(
    n,
    nb,
    prompt_cache,
    prompt_states,
    block_steps,
    prompt_lengths,
    target_slots,
    cache_lengths,
    resident_cache,
    token_cache,
    queries,
    resident_states,
    decay_rates,
    step_sizes,
    inner_input,
    inner_gate,
    state_input,
    state_readout,
    skip_gain,
):
    levels = n.bit_length() - 1
    prompts, block_len, kv_heads, width = prompt_cache.shape
    requests, heads, head_dim = queries.shape
    state_n, channels = decay_rates.shape
    share = channels // n
    piece = share // PIECES
    own_heads = heads // n
    positions = resident_cache.shape[1]
    all_prompts = prompts * nb
    rows = block_len // n
    unit_count = prompts * PIECES
    late_units = LATE
    f32, bf16, i16 = jnp.float32, jnp.bfloat16, jnp.int16
    vmem = pl.BlockSpec(memory_space=pltpu.VMEM)
    hbm = pl.BlockSpec(memory_space=pltpu.HBM)
    dma = pltpu.SemaphoreType.DMA
    halves = [n >> (s + 1) for s in range(levels)]
    through = (resident_states, step_sizes, inner_input, inner_gate, state_input, state_readout, skip_gain[None])
    operands = (
        prompt_cache.reshape(prompts, rows, n, kv_heads, width),
        prompt_states[:, 0],
        block_steps,
        resident_cache[:, :, 0],
        token_cache,
        queries,
        decay_rates,
    ) + through
    outs = (
        pltpu.VMEM((requests, positions, kv_heads, width), bf16),
        pltpu.VMEM((all_prompts, state_n, share), f32),
        pltpu.VMEM((requests, own_heads, head_dim), bf16),
        pltpu.VMEM((state_n, share), f32),
    ) + tuple(pltpu.VMEM(x.shape, x.dtype) for x in through)
    scratch = [
        pltpu.VMEM((nb, n, prompts, rows, kv_heads, width), bf16),
        pltpu.VMEM((prompts, state_n, channels), f32),
        pltpu.VMEM(block_steps.shape, f32),
        pltpu.VMEM((requests, positions, kv_heads, width), bf16),
        pltpu.VMEM(token_cache.shape, bf16),
        pltpu.VMEM(queries.shape, bf16),
        pltpu.VMEM(decay_rates.shape, f32),
        pltpu.VMEM((n, requests * own_heads, head_dim), i16),
        pltpu.VMEM((heads, 128), f32),
        pltpu.VMEM((n, 1, 128), f32),
        pltpu.VMEM((n, requests * own_heads, head_dim), i16),
        pltpu.VMEM((n, 1, 128), f32),
        pltpu.SMEM(prompt_lengths.shape, jnp.int32),
        pltpu.SMEM(target_slots.shape, jnp.int32),
        pltpu.SMEM(cache_lengths.shape, jnp.int32),
        dma((10,)),
        dma((prompts,)),
        dma((len(through),)),
    ]
    for _ in range(2):
        scratch += [pltpu.VMEM((h * prompts, share), i16) for h in halves]
    scratch += [pltpu.VMEM((h, prompts, share), f32) for h in halves]
    scratch += [pltpu.VMEM((h * prompts, share), f32) for h in halves[1:]]
    for _ in range(2):
        scratch += [pltpu.VMEM((unit_count, h, state_n, piece), i16) for h in halves]
    scratch += [pltpu.VMEM((unit_count, h, state_n, piece), f32) for h in halves[1:]]
    scratch += [pltpu.VMEM((n, prompts, 128), f32)]
    scratch += [pltpu.VMEM((levels, prompts, 128), f32)] * 2
    if late_units:
        late_lanes = late_units * piece
        scratch += [pltpu.VMEM((2, 1, 128), f32)] * 2
        scratch += [pltpu.VMEM((n, late_lanes), i16)] * 2
        scratch += [pltpu.VMEM((n, 1, late_lanes), f32)]
        scratch += [pltpu.VMEM((n // 2, late_lanes), i16)] * 2
        scratch += [pltpu.VMEM((n // 2, 1, late_lanes), f32)]
        scratch += [pltpu.VMEM((n // 2, late_lanes), f32)]
        scratch += [dma((2,))] * 2
    scratch += [dma((1,))] * 2
    scratch += [dma((max(nb - 1, 1),))] * 2
    scratch += [dma((levels,))] * 2
    scratch += [dma((levels,)), dma((levels, unit_count))]
    scratch += [dma((1,)), dma((levels,))]
    scratch += [dma((max(nb - 1, 1),))] * 2
    scratch += [dma((1,))] * 4
    scalars = [
        pltpu.with_memory_space_constraint(x, pltpu.HBM)
        for x in (prompt_lengths, target_slots, cache_lengths)
    ]
    parts = pl.pallas_call(
        functools.partial(exchange, (n, nb, levels, block_len, late_units)),
        out_shape=outs,
        in_specs=[hbm] * (3 + len(operands)),
        out_specs=(vmem,) * len(outs),
        scratch_shapes=scratch,
        compiler_params=pltpu.CompilerParams(
            collective_id=0, has_side_effects=True, vmem_limit_bytes=40 << 20
        ),
    )(*scalars, *(pltpu.with_memory_space_constraint(x, pltpu.HBM) for x in operands))
    chunks = share // min(512, share)
    merged, attention, next_states, mamba_output = pl.pallas_call(
        functools.partial(finish, (n, nb)),
        out_shape=(
            jax.ShapeDtypeStruct((requests, positions, kv_heads, width), bf16),
            jax.ShapeDtypeStruct((requests, own_heads, head_dim), bf16),
            jax.ShapeDtypeStruct((requests, state_n, share), f32),
            jax.ShapeDtypeStruct((requests, share), bf16),
        ),
        in_specs=[hbm] * 3 + [vmem] * len(parts),
        out_specs=(hbm,) * 4,
        scratch_shapes=[
            pltpu.VMEM((requests, state_n, share), f32),
            pltpu.VMEM((requests, share), bf16),
            *(pltpu.SMEM(x.shape, jnp.int32) for x in scalars),
            dma((3 + chunks,)),
            dma((3,)),
        ],
        compiler_params=pltpu.CompilerParams(vmem_limit_bytes=16 << 20),
    )(*scalars, *parts)
    return merged[:, :, None], attention, next_states, mamba_output


def solution(mesh):
    n, nb = mesh.shape["seq"], mesh.shape["batch"]
    return jax.shard_map(
        functools.partial(local, n, nb),
        mesh=mesh,
        in_specs=(
            P(("groups", "batch"), "seq", None, None),
            P(("groups", "batch"), "seq", None, None),
            P(("groups", "batch"), "seq", None),
            P("groups"),
            P("groups"),
            P(("groups", "batch")),
            P(("groups", "batch"), None, "seq", None, None),
            P(("groups", "batch"), None, None),
            P(("groups", "batch"), None, None),
            P(("groups", "batch"), None, "seq"),
            P(),
            P(("groups", "batch"), "seq"),
            P(("groups", "batch"), "seq"),
            P(("groups", "batch"), "seq"),
            P(("groups", "batch"), None),
            P(("groups", "batch"), None),
            P("seq"),
        ),
        out_specs=(
            P(("groups", "batch"), None, "seq", None, None),
            P(("groups", "batch"), "seq", None),
            P(("groups", "batch"), None, "seq"),
            P(("groups", "batch"), "seq"),
        ),
        check_vma=False,
    )
```

```python
import functools
import math

import jax
import jax.numpy as jnp
from jax import lax
from jax.experimental import pallas as pl
from jax.experimental.pallas import tpu as pltpu
from jax.sharding import PartitionSpec as P

MESH = pl.DeviceIdType.MESH
FULL = 32760.0
LOW = -1e30
PIECES = 4
LATE = 2
STEP_UNIT = float(1 << 18)
D_TIME, D_GAP = 4.5, 4.6
BOUND_TIME, BOUND_GAP = 6.5, 3.5
RELAY_TIME, ATTEND_TIME, ATTEND_GAP = 14.5, 15.5, 0.5
OUT_TIME, OUT_GAP = 19.5, 0.05
FOLD_TIME, FOLD_GAP, FIRST_LAG, NEXT_LAG = 8.8, 1.39, 5.5, 5.5
LATE_TIME, LATE_GAP, LAST_GAP = 13.0, 0.5, 4.0


def to_int16(value):
    return jnp.round(value).astype(jnp.int32).astype(jnp.int16)


def to_float(value):
    return value.astype(jnp.int32).astype(jnp.float32)


def tile_lanes(row, width):
    return jnp.concatenate([row] * (width // 128), axis=1)


def lane_top(values):
    top = jnp.abs(values[0])
    for value in values[1:]:
        top = jnp.maximum(top, jnp.abs(value))
    parts = [top[:, i : i + 128] for i in range(0, top.shape[1], 128)]
    top = parts[0]
    for part in parts[1:]:
        top = jnp.maximum(top, part)
    return jnp.maximum(jnp.max(top, axis=0, keepdims=True), 1e-30)


def split_rows(value, size, bit):
    count = value.shape[0] // size
    even = [value[k * size : (k + 1) * size] for k in range(0, count, 2)]
    odd = [value[k * size : (k + 1) * size] for k in range(1, count, 2)]
    even = jnp.concatenate(even, axis=0) if len(even) > 1 else even[0]
    odd = jnp.concatenate(odd, axis=0) if len(odd) > 1 else odd[0]
    right = jnp.full(even.shape, bit, jnp.int32) == 1
    return jnp.where(right, odd, even), jnp.where(right, even, odd)


def pick(r, b, requests, all_prompts, plen, tslot, clen):
    slot = b * requests + r
    chosen, length, hits = jnp.int32(0), jnp.int32(0), jnp.int32(0)
    for p in range(all_prompts):
        hit = tslot[p] == slot
        chosen = jnp.where(hit, p, chosen)
        length = jnp.where(hit, plen[p], length)
        hits = jnp.where(hit, 1, hits)
    return chosen, hits, jnp.where(hits > 0, length, clen[r])


def exchange(dims, *refs):
    n, nb, levels, block_len, late_units = dims
    refs = list(refs)

    def take(count):
        out = refs[:count]
        del refs[:count]
        return out

    scalar_hbm = take(3)
    cache_hbm, states_hbm, steps_hbm, resident_hbm, token_hbm, queries_hbm, rates_hbm = take(7)
    through_hbm = take(7)
    merged, handed, attention, rates_own = take(4)
    through = take(7)
    arrived, states, steps, resident, token, queries, rates, osend, lse_all, lse_send = take(10)
    orecv, lse_recv = take(2)
    plen, tslot, clen = scalars = take(3)
    load_sems, state_sems, through_sems = take(3)
    d_send, d_recv, d_sel = take(levels), take(levels), take(levels)
    d_keep = take(levels - 1)
    q_send, q_recv = take(levels), take(levels)
    acc = take(levels - 1)
    table, bound_own, bound_peer = take(3)
    if late_units:
        late_own, late_peer, zsteps_send, zsteps_recv, zpre = take(5)
        zd_send, zd_recv, zd_sel, zd_keep = take(4)
        zd_ss, zd_rs = take(2)
    (
        cache_ss, cache_rs, relay_ss, relay_rs, d_ss, d_rs, q_ss, q_rs, m_ss, m_rs,
        hand_ss, hand_rs, o_ss, o_rs, l_ss, l_rs,
    ) = refs

    me = lax.axis_index("seq")
    b = lax.axis_index("batch")
    prompts, rows, _, kv_heads, width = cache_hbm.shape
    all_prompts = prompts * nb
    requests, heads, head_dim = queries.shape
    state_n, channels = rates.shape
    share_len = channels // n
    piece = share_len // PIECES
    own_heads = heads // n
    group = heads // kv_heads
    positions = resident.shape[1]
    bits = [lax.rem(me // (1 << s), 2) for s in range(levels)]
    peers = [me + (1 - 2 * bits[s]) * (1 << s) for s in range(levels)]
    first = b * prompts

    barrier = pltpu.get_barrier_semaphore()
    for k in range(1, n):
        pl.semaphore_signal(barrier, inc=1, device_id={"seq": lax.rem(me + k, n)}, device_id_type=MESH)
    for k in range(1, nb):
        pl.semaphore_signal(barrier, inc=1, device_id={"batch": lax.rem(b + k, nb)}, device_id_type=MESH)

    def load(src, dst, sem):
        copy = pltpu.make_async_copy(src, dst, sem)
        copy.start()
        return copy

    load_scalars = [load(src, dst, load_sems.at[6 + i]) for i, (src, dst) in enumerate(zip(scalar_hbm, scalars))]
    load_steps = load(steps_hbm, steps, load_sems.at[0])
    load_states = [load(states_hbm.at[0], states.at[0], state_sems.at[0])]
    load_piece = load(cache_hbm.at[:, :, me], arrived.at[b, me], load_sems.at[9])
    load_rates = load(rates_hbm, rates, load_sems.at[1])
    for p in range(1, prompts):
        load_states.append(load(states_hbm.at[p], states.at[p], state_sems.at[p]))
    load_attention = [
        load(resident_hbm, resident, load_sems.at[2]),
        load(token_hbm, token, load_sems.at[3]),
        load(queries_hbm, queries, load_sems.at[4]),
    ]
    own_lanes = pl.ds(pl.multiple_of(me * share_len, 128), share_len)
    load_through = [load(rates_hbm.at[:, own_lanes], rates_own, load_sems.at[5])]
    for i, (src, dst) in enumerate(zip(through_hbm, through)):
        load_through.append(load(src, dst, through_sems.at[i]))

    def remote(src, dst, ss, rs, where):
        return pltpu.make_async_remote_copy(
            src_ref=src, dst_ref=dst, send_sem=ss, recv_sem=rs, device_id=where, device_id_type=MESH
        )

    def start(copy):
        copy.start()
        return copy

    def settle(ref, sem):
        pltpu.make_async_copy(ref, ref, sem).wait()

    def lanes(share, h):
        return pl.ds(pl.multiple_of(share * share_len + h * piece, 128), piece)

    pl.semaphore_wait(barrier, n - 1 + nb - 1)

    def across(k):
        to = me
        for i in range(levels):
            if (k >> i) % 2:
                to = to + peers[i] - me
        return to

    def send_cache(k):
        to = across(k)
        start(remote(cache_hbm.at[:, :, to], arrived.at[b, me], cache_ss.at[0], cache_rs.at[0], {"seq": to}))

    for k in range(n - 1, 1, -2):
        send_cache(k)
    for k in range(n - 2, 0, -2):
        send_cache(k)

    for copy in load_scalars:
        copy.wait()
    usable = [
        jnp.where(me * block_len < plen[first + p], 1.0, 0.0).astype(jnp.float32)
        for p in range(prompts)
    ]

    step_width = min(512, share_len)
    row_id = lax.broadcasted_iota(jnp.int32, (prompts, step_width), 0)
    usable_rows = jnp.zeros((prompts, step_width), jnp.float32)
    for p in range(prompts):
        usable_rows = jnp.where(row_id == p, usable[p], usable_rows)

    def step_rows(bit, c):
        parts = []
        for k in range(n // 2):
            at = pl.ds(pl.multiple_of((2 * k + bit) * share_len + c * step_width, 128), step_width)
            parts.append(jnp.concatenate([steps[p, :, at] for p in range(prompts)], axis=0) * usable_rows)
        return jnp.concatenate(parts, axis=0)

    def columns(c):
        return pl.ds(pl.multiple_of(c * step_width, 128), step_width)

    d_copies = [
        remote(d_send[s], d_recv[s], d_ss.at[s], d_rs.at[s], {"seq": peers[s]}) for s in range(levels)
    ]
    load_steps.wait()

    @pl.loop(0, share_len // step_width)
    def _(c):
        d_send[0][:, columns(c)] = to_int16(step_rows(1 - bits[0], c) * STEP_UNIT)

    start(d_copies[0])

    def fold_steps(s):
        d_copies[s].wait_recv()

        @pl.loop(0, share_len // step_width)
        def _(c):
            at = columns(c)
            other = to_float(d_recv[s][:, at]) * ((1 << s) / STEP_UNIT)
            own = step_rows(bits[0], c) if s == 0 else d_keep[s - 1][:, at]
            selected = jnp.where(jnp.full(own.shape, bits[s], jnp.int32) == 1, own, other)
            for k in range(n >> (s + 1)):
                d_sel[s][k, :, at] = selected[k * prompts : (k + 1) * prompts]
            if s + 1 < levels:
                keep, send = split_rows(own + other, prompts, bits[s + 1])
                d_keep[s][:, at] = keep
                d_send[s + 1][:, at] = to_int16(send * (STEP_UNIT / (1 << (s + 1))))

        if s + 1 < levels:
            start(d_copies[s + 1])

    def bottom(device, s):
        return device - lax.rem(device, 1 << s)

    def fold_bounds(s):
        settle(table.at[pl.ds(0, 1 << s)], m_rs.at[s])

        def group_bound(device):
            total = table[bottom(device, s)]
            for i in range(1, 1 << s):
                total = total + table[bottom(device, s) + i]
            return total

        bound_peer[s] = group_bound(peers[s])
        if s + 1 < levels:
            bound_own[s + 1] = bound_own[s] + bound_peer[s]
        if late_units and s == 1:
            at = slice(late_prompt, late_prompt + 1)
            late_own[1] = table[me, at] + table[peers[1], at]
            late_peer[0] = table[peers[1], at]
            late_peer[1] = table[peers[0], at] + table[peers[0] + peers[1] - me, at]

    half = n // 2
    late_bits = [bits[1], bits[0]] + bits[2:]
    late_peers = [peers[1], peers[0]] + peers[2:]
    units = [(p, h) for p in range(prompts) for h in range(PIECES)]
    total_units = len(units)
    plain = list(range(total_units - late_units))
    late = list(range(total_units - late_units, total_units))
    late_prompt = prompts - 1
    late_from = PIECES - late_units

    def is_late(u):
        return u >= total_units - late_units

    def bit_of(s, u):
        return late_bits[s] if is_late(u) else bits[s]

    def late_share(v):
        return (v // 4) * 4 + (v % 2) * 2 + (v // 2) % 2

    q_copies = {}

    def send_values(s, u, values, factor):
        bound = late_own[s] if is_late(u) and s < 2 else bound_own[s, units[u][0] : units[u][0] + 1]
        scale = tile_lanes(FULL / bound * factor, piece)
        for k, value in enumerate(values):
            q_send[s][u, k] = to_int16(value * scale)
        where = {"seq": (late_peers if is_late(u) else peers)[s]}
        q_copies[s, u] = start(remote(q_send[s].at[u], q_recv[s].at[u], q_ss.at[s], q_rs.at[s, u], where))

    def read(s, u, k):
        p, h = units[u]
        if s > 0:
            return acc[s - 1][u, k]
        if is_late(u):
            return late_value(u, 2 * k + late_bits[0])
        return states[p, :, lanes(2 * k + bits[0], h)] * usable[p]

    def first_send(u):
        p, h = units[u]
        if is_late(u):
            send_values(0, u, [late_value(u, 2 * k + 1 - late_bits[0]) for k in range(half)], 1.0)
        else:
            values = [states[p, :, lanes(2 * k + 1 - bits[0], h)] for k in range(half)]
            send_values(0, u, values, usable[p])

    def fold(s, u):
        p, h = units[u]
        q_copies[s, u].wait_recv()
        bound = late_peer[s] if is_late(u) and s < 2 else bound_peer[s, p : p + 1]
        scale = tile_lanes(bound * (1.0 / FULL), piece)
        right = jnp.full((state_n, piece), bit_of(s, u), jnp.int32) == 1
        below = lax.rem(late_share(me) if is_late(u) else me, 1 << (s + 1))

        def folded(k):
            other = to_float(q_recv[s][u, k]) * scale
            own = read(s, u, k)
            if is_late(u) and s == 1:
                return own + other
            v = k * (1 << (s + 1)) + below
            share = late_share(v) if is_late(u) else v
            if is_late(u) and s == 0:
                late_at = (h - late_from) * piece
                behind = zd_sel[k][:, late_at : late_at + piece]
            else:
                behind = d_sel[s][k, p : p + 1, h * piece : (h + 1) * piece]
            decay = jnp.exp(-rates[:, lanes(share, h)] * behind)
            early = jnp.where(right, other, own)
            later = jnp.where(right, own, other)
            return decay * early + later

        if s + 1 < levels:
            bit = bit_of(s + 1, u)
            count = n >> (s + 2)
            send_values(s + 1, u, [folded(2 * k + 1 - bit) for k in range(count)], 1.0)
            for k in range(count):
                acc[s][u, k] = folded(2 * k + bit)
        else:
            at = pl.ds(h * piece, piece)
            handed[first + p, :, at] = folded(0)
            for k in range(1, nb):
                start(
                    remote(
                        handed.at[first + p, :, at],
                        handed.at[first + p, :, at],
                        hand_ss.at[k - 1],
                        hand_rs.at[k - 1],
                        {"batch": lax.rem(b + k, nb)},
                    )
                )

    if late_units:
        late_lanes = late_units * piece

        def late_row(v):
            at = late_share(v) * share_len + late_from * piece
            return steps[late_prompt, :, at : at + late_lanes]

        def late_rows():
            return jnp.concatenate([late_row(v) for v in range(n)], axis=0) * usable[late_prompt]

        zd_copies = [
            remote(zsteps_send, zsteps_recv, zd_ss.at[0], zd_rs.at[0], {"seq": peers[0]}),
            remote(zd_send, zd_recv, zd_ss.at[1], zd_rs.at[1], {"seq": late_peers[0]}),
        ]
        zsteps_send[...] = to_int16(late_rows() * STEP_UNIT)
        start(zd_copies[0])

        def late_value(u, v):
            h = units[u][1]
            at = lanes(late_share(v), h)
            late_at = (h - late_from) * piece
            decay = jnp.exp(-rates[:, at] * zpre[v][:, late_at : late_at + piece])
            return states[late_prompt, :, at] * (decay * usable[late_prompt])

        def late_begin():
            zd_copies[0].wait_recv()
            other = to_float(zsteps_recv[...]) * (1.0 / STEP_UNIT)
            before = jnp.where(jnp.full(other.shape, bits[0], jnp.int32) == 1, 0.0, other)
            for v in range(n):
                zpre[v] = before[v : v + 1]
            keep, send = split_rows(late_rows() + other, 1, late_bits[0])
            zd_keep[...] = keep
            zd_send[...] = to_int16(send * (STEP_UNIT / 2))
            start(zd_copies[1])

            late_own[0] = bound_own[0, late_prompt : late_prompt + 1]
            for u in late:
                first_send(u)

        def late_steps():
            zd_copies[1].wait_recv()
            own, other = zd_keep[...], to_float(zd_recv[...]) * (2 / STEP_UNIT)
            selected = jnp.where(jnp.full(own.shape, late_bits[0], jnp.int32) == 1, own, other)
            for k in range(half):
                zd_sel[k] = selected[k : k + 1]


    relays = [
        remote(
            arrived.at[b], arrived.at[b], relay_ss.at[k - 1], relay_rs.at[k - 1], {"batch": lax.rem(b + k, nb)}
        )
        for k in range(1, nb)
    ]

    top_width = min(512, share_len)
    for p in range(prompts):
        load_states[p].wait()

        def larger(i, top):
            at = pl.ds(pl.multiple_of(i * top_width, 128), top_width)
            return jnp.maximum(top, jnp.abs(states[p, :, at]))

        top = lax.fori_loop(0, channels // top_width, larger, jnp.zeros((state_n, top_width), jnp.float32), unroll=4)
        bound_own[0, p : p + 1] = jnp.maximum(lane_top([top]) * usable[p], 1e-30)
    table[me] = bound_own[0]
    for s in range(levels):
        for i in range(1 << s):
            to = bottom(peers[s], s) + i
            start(remote(bound_own.at[0], table.at[me], m_ss.at[0], m_rs.at[s], {"seq": to}))
    send_cache(1)
    for u in plain:
        first_send(u)

    shape3 = (positions, kv_heads, width)
    position = lax.broadcasted_iota(jnp.int32, shape3, 0) * n + me
    flat = positions * kv_heads
    column = lax.broadcasted_iota(jnp.int32, (heads, flat), 1)
    owner = lax.broadcasted_iota(jnp.int32, (heads, flat), 0) // group
    same_head = lax.rem(column, kv_heads) == owner
    column_position = (column // kv_heads) * n + me
    note_lane = lax.broadcasted_iota(jnp.int32, (heads, 128), 1)
    note_lane = note_lane - lax.rem(lax.broadcasted_iota(jnp.int32, (heads, 128), 0), own_heads)

    def attend(r):
        chosen, hits, length = pick(r, b, requests, all_prompts, plen, tslot, clen)
        fresh_limit = jnp.where(hits > 0, length, 0)
        new = arrived[chosen // prompts, :, lax.rem(chosen, prompts)].reshape(shape3).astype(jnp.float32)
        old = resident[r].astype(jnp.float32)
        x = jnp.where(position < fresh_limit, new, old)
        x = jnp.where(position < length, x, 0.0)
        x = jnp.where(position == length, token[r].astype(jnp.float32)[None], x)
        merged[r] = x.astype(jnp.bfloat16)
        x2 = x.reshape(flat, width)
        keys = x2[:, :head_dim].astype(jnp.bfloat16)
        values = x2[:, head_dim:].astype(jnp.bfloat16)
        score = lax.dot_general(
            queries[r], keys, (((1,), (1,)), ((), ())), preferred_element_type=jnp.float32
        ) * (1.0 / math.sqrt(head_dim))
        seen = same_head & (column_position <= length)
        score = jnp.where(seen, score, LOW)
        top = jnp.max(score, axis=1, keepdims=True)
        weight = jnp.where(seen, jnp.exp(score - top), 0.0)
        total = jnp.sum(weight, axis=1, keepdims=True)
        out = jnp.dot(weight.astype(jnp.bfloat16), values, preferred_element_type=jnp.float32)
        some = total > 0.0
        safe = jnp.where(some, total, 1.0)
        out = out / safe
        lse = jnp.where(some, top + jnp.log(safe), LOW)
        peak = jnp.maximum(jnp.max(jnp.abs(out), axis=1, keepdims=True), 1e-30)
        coded = jnp.round(out * (FULL / peak)).astype(jnp.int32)
        for j in range(n):
            osend[j, r * own_heads : (r + 1) * own_heads] = coded[j * own_heads : (j + 1) * own_heads].astype(jnp.int16)
        noted = jnp.where(note_lane == r * own_heads, lse, lse_all[...])
        lse_all[...] = jnp.where(note_lane == (requests + r) * own_heads, peak * (1.0 / FULL), noted)

    def attention_begin():
        settle(arrived.at[b, pl.ds(0, n - 1)], cache_rs.at[0])
        load_piece.wait()
        for copy in relays:
            start(copy)
        for copy in load_attention:
            copy.wait()
        lse_all[...] = jnp.zeros((heads, 128), jnp.float32)

    def send_out(ks):
        for k in ks:
            to = across(k)
            lse_send[to] = jnp.sum(lse_all[pl.ds(pl.multiple_of(to * own_heads, own_heads), own_heads)], axis=0, keepdims=True)
            start(remote(lse_send.at[to], lse_recv.at[me], l_ss.at[0], l_rs.at[0], {"seq": to}))
            start(remote(osend.at[to], orecv.at[me], o_ss.at[0], o_rs.at[0], {"seq": to}))

    def attention_end():
        send_out(range(n - 2, 0, -2))
        lse_recv[me] = jnp.sum(lse_all[pl.ds(pl.multiple_of(me * own_heads, own_heads), own_heads)], axis=0, keepdims=True)
        orecv[me] = osend[me]

    def attention_last():
        send_out(range(n - 1, 0, -2))

    load_rates.wait()

    def attend_some(r):
        if r == 0:
            for copy in relays:
                copy.wait_recv()
        attend(r)

    events = [(D_TIME + D_GAP * s, functools.partial(fold_steps, s)) for s in range(levels)]
    events += [(BOUND_TIME + BOUND_GAP * s, functools.partial(fold_bounds, s)) for s in range(levels)]
    events.append((RELAY_TIME, attention_begin))
    events.append((OUT_TIME, attention_end))
    events.append((OUT_TIME + OUT_GAP, attention_last))
    events += [(ATTEND_TIME + ATTEND_GAP * r, functools.partial(attend_some, r)) for r in range(requests)]
    for i, u in enumerate(plain):
        for s in range(levels):
            lag = FIRST_LAG + NEXT_LAG * (s - 1) if s else 0.0
            events.append((FOLD_TIME + FOLD_GAP * i + lag, functools.partial(fold, s, u)))
    if late_units:
        events.append((D_TIME + 0.1, late_begin))
        events.append((D_TIME + D_GAP + 0.1, late_steps))
        for i, u in enumerate(late):
            events.append((LATE_TIME + 0.1 * i, functools.partial(fold, 0, u)))
            for s in range(1, levels):
                expected = FOLD_TIME + FOLD_GAP * (len(plain) + i / 2) + LATE_GAP + LAST_GAP * (s - 1)
                events.append((expected, functools.partial(fold, s, u)))
    for _, event in sorted(events, key=lambda e: e[0]):
        event()

    for copy in load_through:
        copy.wait()
    others = pl.ds(0, n - 1)
    settle(lse_recv.at[others], l_rs.at[0])
    settle(orecv.at[others], o_rs.at[0])
    head_lane = lax.broadcasted_iota(jnp.int32, (n, own_heads, 128), 2)
    head_lane = head_lane - lax.broadcasted_iota(jnp.int32, (n, own_heads, 128), 1)
    noted = jnp.broadcast_to(lse_recv[...], (n, own_heads, 128))
    for r in range(requests):
        lse = jnp.sum(jnp.where(head_lane == r * own_heads, noted, 0.0), axis=2, keepdims=True)
        unit = jnp.sum(jnp.where(head_lane == (requests + r) * own_heads, noted, 0.0), axis=2, keepdims=True)
        share = jnp.exp(lse - jnp.max(lse, axis=0, keepdims=True))
        parts = to_float(orecv[:, r * own_heads : (r + 1) * own_heads])
        top = jnp.sum(share * unit * parts, axis=0)
        attention[r] = (top / jnp.sum(share, axis=0)).astype(jnp.bfloat16)
    for k in range(1, nb):
        theirs = pl.ds(lax.rem(b + nb - k, nb) * prompts, prompts)
        settle(handed.at[theirs], hand_rs.at[k - 1])
        settle(handed.at[pl.ds(first, prompts)], hand_ss.at[k - 1])
    settle(arrived.at[b, others], cache_ss.at[0])
    settle(lse_send.at[others], l_ss.at[0])
    settle(osend.at[others], o_ss.at[0])
    for s in range(levels):
        settle(q_send[s], q_ss.at[s])
    settle(table.at[others], m_ss.at[0])
    for copy in relays + d_copies + (zd_copies if late_units else []):
        copy.wait_send()


def finish(dims, plen_hbm, tslot_hbm, clen_hbm, merged, handed, attention, rates, rstates, dt, inner, gate, s_in, s_out, skip,
           merged_out, attention_out, nstates_out, mout_out, nstates, mout, plen, tslot, clen, sems, scalar_sems):
    n, nb = dims
    b = lax.axis_index("batch")
    all_prompts = handed.shape[0]
    requests, state_n, share_len = rstates.shape
    chunk = min(512, share_len)
    per_share = share_len // chunk

    scalar_copies = []
    for i, (src, dst) in enumerate(((plen_hbm, plen), (tslot_hbm, tslot), (clen_hbm, clen))):
        scalar_copies.append(pltpu.make_async_copy(src, dst, scalar_sems.at[i]))
        scalar_copies[-1].start()
    copies = []

    def out(src, dst, i):
        copy = pltpu.make_async_copy(src, dst, sems.at[i])
        copy.start()
        copies.append(copy)

    out(merged, merged_out, 0)
    out(attention, attention_out, 2)
    eye = lax.broadcasted_iota(jnp.int32, (state_n, state_n), 0) == lax.broadcasted_iota(
        jnp.int32, (state_n, state_n), 1
    )

    def as_column(row):
        spread = jnp.where(eye, jnp.broadcast_to(row, (state_n, state_n)), 0.0)
        return jnp.sum(spread, axis=1, keepdims=True)

    in_all, out_all = s_in[...], s_out[...]
    in_cols = [as_column(in_all[r : r + 1]) for r in range(requests)]
    out_cols = [as_column(out_all[r : r + 1]) for r in range(requests)]
    for c in range(per_share):
        at = pl.ds(c * chunk, chunk)
        step_rows = dt[:, at]
        rate = -rates[:, at]
        for r in range(requests):
            nstates[r, :, at] = jnp.exp(rate * step_rows[r : r + 1])

    for copy in scalar_copies:
        copy.wait()
    picks = [pick(r, b, requests, all_prompts, plen, tslot, clen) for r in range(requests)]

    for c in range(per_share):
        at = pl.ds(c * chunk, chunk)
        step_rows = dt[:, at]
        x_rows = inner[:, at].astype(jnp.float32)
        g = gate[:, at].astype(jnp.float32)
        push_rows = step_rows * x_rows
        out_rows = []
        for r in range(requests):
            chosen, hits, _ = picks[r]
            fresh = jnp.full((state_n, chunk), hits, jnp.int32) > 0
            begin = jnp.where(fresh, handed[chosen, :, at], rstates[r, :, at])
            after = nstates[r, :, at] * begin
            after = after + push_rows[r : r + 1] * in_cols[r]
            nstates[r, :, at] = after
            out_rows.append(jnp.sum(out_cols[r] * after, axis=0, keepdims=True))
        out(nstates.at[:, :, at], nstates_out.at[:, :, at], 3 + c)
        read_out = jnp.concatenate(out_rows, axis=0) + skip[:, at] * x_rows
        mout[:, at] = (read_out * (g / (1.0 + jnp.exp(-g)))).astype(jnp.bfloat16)
    out(mout, mout_out, 1)

    for copy in copies:
        copy.wait()


def local(
    n,
    nb,
    prompt_cache,
    prompt_states,
    block_steps,
    prompt_lengths,
    target_slots,
    cache_lengths,
    resident_cache,
    token_cache,
    queries,
    resident_states,
    decay_rates,
    step_sizes,
    inner_input,
    inner_gate,
    state_input,
    state_readout,
    skip_gain,
):
    levels = n.bit_length() - 1
    prompts, block_len, kv_heads, width = prompt_cache.shape
    requests, heads, head_dim = queries.shape
    state_n, channels = decay_rates.shape
    share = channels // n
    piece = share // PIECES
    own_heads = heads // n
    positions = resident_cache.shape[1]
    all_prompts = prompts * nb
    rows = block_len // n
    unit_count = prompts * PIECES
    late_units = LATE
    f32, bf16, i16 = jnp.float32, jnp.bfloat16, jnp.int16
    vmem = pl.BlockSpec(memory_space=pltpu.VMEM)
    hbm = pl.BlockSpec(memory_space=pltpu.HBM)
    dma = pltpu.SemaphoreType.DMA
    halves = [n >> (s + 1) for s in range(levels)]
    through = (resident_states, step_sizes, inner_input, inner_gate, state_input, state_readout, skip_gain[None])
    operands = (
        prompt_cache.reshape(prompts, rows, n, kv_heads, width),
        prompt_states[:, 0],
        block_steps,
        resident_cache[:, :, 0],
        token_cache,
        queries,
        decay_rates,
    ) + through
    outs = (
        pltpu.VMEM((requests, positions, kv_heads, width), bf16),
        pltpu.VMEM((all_prompts, state_n, share), f32),
        pltpu.VMEM((requests, own_heads, head_dim), bf16),
        pltpu.VMEM((state_n, share), f32),
    ) + tuple(pltpu.VMEM(x.shape, x.dtype) for x in through)
    scratch = [
        pltpu.VMEM((nb, n, prompts, rows, kv_heads, width), bf16),
        pltpu.VMEM((prompts, state_n, channels), f32),
        pltpu.VMEM(block_steps.shape, f32),
        pltpu.VMEM((requests, positions, kv_heads, width), bf16),
        pltpu.VMEM(token_cache.shape, bf16),
        pltpu.VMEM(queries.shape, bf16),
        pltpu.VMEM(decay_rates.shape, f32),
        pltpu.VMEM((n, requests * own_heads, head_dim), i16),
        pltpu.VMEM((heads, 128), f32),
        pltpu.VMEM((n, 1, 128), f32),
        pltpu.VMEM((n, requests * own_heads, head_dim), i16),
        pltpu.VMEM((n, 1, 128), f32),
        pltpu.SMEM(prompt_lengths.shape, jnp.int32),
        pltpu.SMEM(target_slots.shape, jnp.int32),
        pltpu.SMEM(cache_lengths.shape, jnp.int32),
        dma((10,)),
        dma((prompts,)),
        dma((len(through),)),
    ]
    for _ in range(2):
        scratch += [pltpu.VMEM((h * prompts, share), i16) for h in halves]
    scratch += [pltpu.VMEM((h, prompts, share), f32) for h in halves]
    scratch += [pltpu.VMEM((h * prompts, share), f32) for h in halves[1:]]
    for _ in range(2):
        scratch += [pltpu.VMEM((unit_count, h, state_n, piece), i16) for h in halves]
    scratch += [pltpu.VMEM((unit_count, h, state_n, piece), f32) for h in halves[1:]]
    scratch += [pltpu.VMEM((n, prompts, 128), f32)]
    scratch += [pltpu.VMEM((levels, prompts, 128), f32)] * 2
    if late_units:
        late_lanes = late_units * piece
        scratch += [pltpu.VMEM((2, 1, 128), f32)] * 2
        scratch += [pltpu.VMEM((n, late_lanes), i16)] * 2
        scratch += [pltpu.VMEM((n, 1, late_lanes), f32)]
        scratch += [pltpu.VMEM((n // 2, late_lanes), i16)] * 2
        scratch += [pltpu.VMEM((n // 2, 1, late_lanes), f32)]
        scratch += [pltpu.VMEM((n // 2, late_lanes), f32)]
        scratch += [dma((2,))] * 2
    scratch += [dma((1,))] * 2
    scratch += [dma((max(nb - 1, 1),))] * 2
    scratch += [dma((levels,))] * 2
    scratch += [dma((levels,)), dma((levels, unit_count))]
    scratch += [dma((1,)), dma((levels,))]
    scratch += [dma((max(nb - 1, 1),))] * 2
    scratch += [dma((1,))] * 4
    scalars = [
        pltpu.with_memory_space_constraint(x, pltpu.HBM)
        for x in (prompt_lengths, target_slots, cache_lengths)
    ]
    parts = pl.pallas_call(
        functools.partial(exchange, (n, nb, levels, block_len, late_units)),
        out_shape=outs,
        in_specs=[hbm] * (3 + len(operands)),
        out_specs=(vmem,) * len(outs),
        scratch_shapes=scratch,
        compiler_params=pltpu.CompilerParams(
            collective_id=0, has_side_effects=True, vmem_limit_bytes=40 << 20
        ),
    )(*scalars, *(pltpu.with_memory_space_constraint(x, pltpu.HBM) for x in operands))
    chunks = share // min(512, share)
    merged, attention, next_states, mamba_output = pl.pallas_call(
        functools.partial(finish, (n, nb)),
        out_shape=(
            jax.ShapeDtypeStruct((requests, positions, kv_heads, width), bf16),
            jax.ShapeDtypeStruct((requests, own_heads, head_dim), bf16),
            jax.ShapeDtypeStruct((requests, state_n, share), f32),
            jax.ShapeDtypeStruct((requests, share), bf16),
        ),
        in_specs=[hbm] * 3 + [vmem] * len(parts),
        out_specs=(hbm,) * 4,
        scratch_shapes=[
            pltpu.VMEM((requests, state_n, share), f32),
            pltpu.VMEM((requests, share), bf16),
            *(pltpu.SMEM(x.shape, jnp.int32) for x in scalars),
            dma((3 + chunks,)),
            dma((3,)),
        ],
        compiler_params=pltpu.CompilerParams(vmem_limit_bytes=16 << 20),
    )(*scalars, *parts)
    return merged[:, :, None], attention, next_states, mamba_output


def solution(mesh):
    n, nb = mesh.shape["seq"], mesh.shape["batch"]
    return jax.shard_map(
        functools.partial(local, n, nb),
        mesh=mesh,
        in_specs=(
            P(("groups", "batch"), "seq", None, None),
            P(("groups", "batch"), "seq", None, None),
            P(("groups", "batch"), "seq", None),
            P("groups"),
            P("groups"),
            P(("groups", "batch")),
            P(("groups", "batch"), None, "seq", None, None),
            P(("groups", "batch"), None, None),
            P(("groups", "batch"), None, None),
            P(("groups", "batch"), None, "seq"),
            P(),
            P(("groups", "batch"), "seq"),
            P(("groups", "batch"), "seq"),
            P(("groups", "batch"), "seq"),
            P(("groups", "batch"), None),
            P(("groups", "batch"), None),
            P("seq"),
        ),
        out_specs=(
            P(("groups", "batch"), None, "seq", None, None),
            P(("groups", "batch"), "seq", None),
            P(("groups", "batch"), None, "seq"),
            P(("groups", "batch"), "seq"),
        ),
        check_vma=False,
    )
```
